128 devices in a mesh: row: 16 (over x_lo, z, core), col: 8 (over x_hi, y).
Axes of the slice: x: 4 (x_hi: 2, x_lo: 2; x = x_hi * 2 + x_lo), y: 4, z: 4, core: 2. Of those that a mesh axis runs over, the one named last changes fastest.
Arguments:
- psi: bfloat16 [4096, 4096], P(('row', 'col')), may hold values from -6 to 6
- hpsi: bfloat16 [4096, 4096], P(('row', 'col')), may hold values from -0.09375 to 0.09375
- eigvec: bfloat16 [2, 16, 128, 4, 8, 128], P(None, 'row', None, None, 'col'), may hold values from -0.09375 to 0.09375
Outputs:
- correlation_tiles: float32 [2, 16, 128, 4, 8, 128], P(None, 'row', None, None, 'col')
- updated_tiles: float32 [2, 16, 128, 4, 8, 128], P(None, 'row', None, None, 'col')
- diag_part: float32 [16], replicated
- offdiag_part: float32 [16], replicated
- rotated: bfloat16 [4096, 4, 8, 128], P('row', None, 'col')
The draws below stay inside these ranges and needn't reach their ends.
All inputs are finite; a program needn't handle non-finite values.
Results may differ from the reference program's by a relative error of at most 0.001.
Values may be sent and summed in bfloat16 or wider, within the bound.
No kernel may reach another device: no remote copies, remote signals or barrier semaphores. Data moves between devices by JAX's collectives and lax.ppermute only.
A program may use at most 128 MiB of HBM per device.

```python
import jax
import jax.numpy as jnp
from jax import lax

NB = 4096
TB = 128
PB = 16
NG = 4096
KR = 2
KC = 4
N_ROW = 16
N_COL = 8


def block_levels(key, shape, pieces, least, largest):
    def one(position, shards_of):
        heights = jax.random.uniform(jax.random.fold_in(jax.random.fold_in(key, 6), position), (shards_of,), jnp.float32, least / len(pieces), largest / len(pieces))
        return jnp.repeat(jnp.exp(heights), shape[position] // shards_of).reshape((-1,) + (1,) * (len(shape) - position - 1))

    loudness = one(*pieces[0])
    for cut in pieces[1:]:
        loudness = loudness * one(*cut)
    return loudness


def centred(rng, dims, spread, most, pieces=(), held_as=jnp.bfloat16):
    array = jax.random.normal(rng, dims, jnp.float32) * spread
    if len(pieces) > 0:
        array = block_levels(rng, dims, pieces, -0.22, 0.18) * array
    return jnp.clip(array, min=-most, max=most).astype(held_as)


def setup_inputs(seed: int = 0) -> dict:
    splits = jax.random.split(jax.random.key(seed), 4)
    psi = centred(splits[0], (NG, NB), 1.0, 6.0, ((0, 128),))
    hpsi = centred(splits[1], (NG, NB), NG ** -0.5, 0.09375, ((0, 128),))
    eigvec = centred(splits[2], (KR, N_ROW, TB, KC, N_COL, TB), NB ** -0.5, 0.09375, ((1, 16), (4, 8)))
    return dict(psi=psi, hpsi=hpsi, eigvec=eigvec)


def reference(psi, hpsi, eigvec):
    highest = lax.Precision.HIGHEST
    mixed = jnp.dot(psi.T, hpsi, preferred_element_type=jnp.float32)
    reduced = 0.5 * (mixed + mixed.T)
    correlation = jnp.dot(psi.T, psi, preferred_element_type=jnp.float32) / float(NG)
    panel = reduced[:, :PB]
    positions = jnp.arange(NB)
    vecs = jnp.zeros((NB, PB), jnp.float32)
    images = jnp.zeros((NB, PB), jnp.float32)
    diag_list = []
    off_list = []
    for step in range(PB):
        column = panel[:, step] - jnp.dot(vecs, images[step], precision=highest) - jnp.dot(images, vecs[step], precision=highest)
        pivot = column[step + 1]
        below = positions > step + 1
        tail = jnp.sum(jnp.where(below, column * column, 0.0))
        length = jnp.sqrt(pivot * pivot + tail)
        beta = jnp.where(pivot >= 0.0, -length, length)
        tau = (beta - pivot) / beta
        vector = jnp.where(positions == step + 1, 1.0, jnp.where(below, column / (pivot - beta), 0.0))
        image = jnp.dot(reduced, vector, precision=highest)
        image = image - jnp.dot(vecs, jnp.dot(vector, images, precision=highest), precision=highest)
        image = image - jnp.dot(images, jnp.dot(vector, vecs, precision=highest), precision=highest)
        image = tau * image
        image = image - 0.5 * tau * jnp.dot(image, vector, precision=highest) * vector
        vecs = vecs.at[:, step].set(vector)
        images = images.at[:, step].set(image)
        diag_list.append(column[step])
        off_list.append(beta)
    updated = reduced - jnp.dot(vecs, images.T, precision=highest) - jnp.dot(images, vecs.T, precision=highest)
    rotation = eigvec.reshape(NB, NB)
    rotated = jnp.dot(psi, rotation, preferred_element_type=jnp.float32).astype(jnp.bfloat16)
    tile_shape = (KR, N_ROW, TB, KC, N_COL, TB)
    return (correlation.reshape(tile_shape), updated.reshape(tile_shape), jnp.stack(diag_list).astype(jnp.float32), jnp.stack(off_list).astype(jnp.float32), rotated.reshape(NG, KC, N_COL, TB))
```

```python
import jax
import jax.numpy as jnp
from jax import lax
from jax.experimental import pallas as pl
from jax.experimental.pallas import tpu as pltpu
from jax.sharding import PartitionSpec as P

PB = 16
LANES = 128
F32 = jnp.float32


def total(x):
    return jnp.sum(jnp.sum(x, axis=-2, keepdims=True), axis=-1, keepdims=True)


def finish_image(recv, vecs, images, vector, tau, tiles):
    half = tiles // 2
    sums = jnp.sum(recv, axis=1)
    image = jnp.concatenate([sums[:, :LANES], sums[:, LANES:]], axis=0).reshape(1, 2 * half, LANES)
    along_w = total(images * vector)
    along_v = total(vecs * vector)
    image = image - jnp.sum(vecs * along_w + images * along_v, axis=0, keepdims=True)
    image = tau * image
    return image - 0.5 * tau * total(image * vector) * vector


def place(into, what, slot):
    slots = lax.broadcasted_iota(jnp.int32, (PB, 1, 1), 0)
    return jnp.where(slots == slot, what, into)


def step_body(
    step_ref, recv_ref, panel_ref, vecs_ref, images_ref, marks_ref, matrix_ref,
    vecs_out, images_out, marks_out, send_out, matrix_vmem, sem,
):
    step = step_ref[0]
    tiles = panel_ref.shape[1]
    copy = pltpu.make_async_copy(matrix_ref, matrix_vmem, sem)
    copy.start()
    lane = lax.broadcasted_iota(jnp.int32, (1, 1, LANES), 2)
    marks = marks_ref[...]
    vecs = vecs_ref[...]
    images = images_ref[...]
    before = jnp.maximum(step - 1, 0)
    vector = vecs_ref[pl.ds(before, 1)]
    tau = marks[2:3, 0:1].reshape(1, 1, 1)
    image = finish_image(recv_ref[...], vecs, images, vector, tau, tiles)
    images = place(images, image, step - 1)
    images_out[...] = images
    head_w = jnp.sum(jnp.where(lane == step, images[:, 0:1, :], 0.0), axis=-1, keepdims=True)
    head_v = jnp.sum(jnp.where(lane == step, vecs[:, 0:1, :], 0.0), axis=-1, keepdims=True)
    column = panel_ref[pl.ds(step, 1)] - jnp.sum(
        vecs * head_w + images * head_v, axis=0, keepdims=True
    )
    shape = (1, tiles, LANES)
    positions = lax.broadcasted_iota(jnp.int32, shape, 1) * LANES + lax.broadcasted_iota(
        jnp.int32, shape, 2
    )
    below = positions > step + 1
    pivot = total(jnp.where(positions == step + 1, column, 0.0))
    tail = total(jnp.where(below, column * column, 0.0))
    corner = total(jnp.where(positions == step, column, 0.0))
    length = jnp.sqrt(pivot * pivot + tail)
    beta = jnp.where(pivot >= 0.0, -length, length)
    tau = (beta - pivot) / beta
    vector = jnp.where(positions == step + 1, 1.0, jnp.where(below, column / (pivot - beta), 0.0))
    vecs_out[...] = place(vecs, vector, step)
    row = lax.broadcasted_iota(jnp.int32, marks.shape, 0)
    spot = lax.broadcasted_iota(jnp.int32, marks.shape, 1) == step
    flat = marks.shape
    marks = jnp.where((row == 0) & spot, jnp.broadcast_to(corner[0], flat), marks)
    marks = jnp.where((row == 1) & spot, jnp.broadcast_to(beta[0], flat), marks)
    marks_out[...] = jnp.where(row == 2, jnp.broadcast_to(tau[0], flat), marks)
    copy.wait()
    col_count, height, width = matrix_vmem.shape
    col_tiles = width // LANES
    sums = jnp.zeros((height, LANES), F32)
    for c in range(col_count):
        for a in range(col_tiles):
            u = a * col_count + c
            sums = sums + matrix_vmem[c, :, a * LANES : (a + 1) * LANES] * vector[0, u : u + 1, :]
    pieces = [
        jnp.sum(sums[k * LANES : (k + 1) * LANES].T, axis=0, keepdims=True)
        for k in range(height // LANES)
    ]
    send_out[...] = jnp.broadcast_to(jnp.concatenate(pieces, axis=1), send_out.shape)


def last_body(
    where_ref, recv_ref, vecs_ref, images_ref, marks_ref, tile_ref, updated_out, vecs_vmem, images_vmem
):
    tiles = vecs_ref.shape[1]
    vecs = vecs_ref[...]
    vector = vecs_ref[PB - 1 : PB]
    tau = marks_ref[2:3, 0:1].reshape(1, 1, 1)
    image = finish_image(recv_ref[...], vecs, images_ref[...], vector, tau, tiles)
    images = place(images_ref[...], image, PB - 1)
    images_vmem[...] = images
    vecs_vmem[...] = vecs
    row_id = where_ref[0]
    col_id = where_ref[1]
    height, width = tile_ref.shape
    row_tiles = height // LANES
    col_tiles = width // LANES

    def part(ref, at):
        return ref[:, pl.ds(at, 1), :].reshape(PB, LANES)

    lefts = [
        jnp.concatenate([part(vecs_vmem, at), part(images_vmem, at)], axis=0)
        for at in (row_id + k * (tiles // row_tiles) for k in range(row_tiles))
    ]
    rights = [
        jnp.concatenate([part(images_vmem, at), part(vecs_vmem, at)], axis=0)
        for at in (col_id + k * (tiles // col_tiles) for k in range(col_tiles))
    ]
    left = jnp.concatenate(lefts, axis=1)
    right = jnp.concatenate(rights, axis=1)
    change = lax.dot_general(
        left, right, (((0,), (0,)), ((), ())),
        precision=lax.Precision.HIGHEST, preferred_element_type=F32,
    )
    updated_out[...] = tile_ref[...] - change


def vmem():
    return pl.BlockSpec(memory_space=pltpu.VMEM)


def on_device(psi, hpsi, eigvec):
    g_rows, bands = psi.shape
    row_tiles, _, tile_size, col_tiles = eigvec.shape[:4]
    row_count = lax.axis_size("row")
    col_count = lax.axis_size("col")
    devices = row_count * col_count
    row_id = lax.axis_index("row")
    col_id = lax.axis_index("col")
    gvecs = g_rows * devices
    height = row_tiles * tile_size
    width = col_tiles * tile_size
    tiles = bands // tile_size

    both = lax.all_gather(jnp.stack([psi, hpsi]), "row")
    k = row_count * 2 * g_rows
    flat = both.reshape(k, bands)
    mine = lax.dynamic_index_in_dim(
        both.reshape(row_count, 2, g_rows, row_tiles, row_count, tile_size), row_id, 4, keepdims=False
    ).reshape(row_count, 2, g_rows, height)
    head = both[:, :, :, :PB]
    only_psi = mine * jnp.array([1, 0], mine.dtype).reshape(1, 2, 1, 1)
    left = jnp.concatenate([mine[:, ::-1], head[:, ::-1], only_psi], axis=3).reshape(
        k, 2 * height + PB
    )
    mixed = lax.dot_general(
        left, flat.reshape(k, col_tiles, col_count, tile_size),
        (((0,), (0,)), ((), ())), preferred_element_type=F32,
    )
    mixed = jnp.transpose(mixed, (2, 0, 1, 3)).reshape(col_count, 2 * height + PB, width)
    matrix = 0.5 * mixed[:, :height]
    strip = 0.5 * mixed[:, height : height + PB]
    overlap = mixed[:, height + PB :] * (1.0 / gvecs)

    strip = jnp.sum(lax.all_to_all(strip, "col", 0, 0, tiled=True), axis=0)
    strip = lax.all_to_all(
        jnp.broadcast_to(strip[None], (col_count, *strip.shape)), "col", 0, 0, tiled=True
    )
    panel = jnp.transpose(
        strip.reshape(col_count, PB, col_tiles, tile_size), (1, 2, 0, 3)
    ).reshape(PB, tiles, tile_size)

    reduced = lax.psum_scatter(
        jnp.concatenate([matrix, overlap], axis=1), "col", scatter_dimension=0, tiled=False
    )

    state = jax.ShapeDtypeStruct((PB, tiles, tile_size), F32)
    marks_shape = jax.ShapeDtypeStruct((8, tile_size), F32)
    advance = pl.pallas_call(
        step_body,
        out_shape=(state, state, marks_shape, jax.ShapeDtypeStruct((devices, height), F32)),
        in_specs=[pl.BlockSpec(memory_space=pltpu.SMEM)]
        + [vmem() for _ in range(5)]
        + [pl.BlockSpec(memory_space=pltpu.HBM)],
        out_specs=tuple(vmem() for _ in range(4)),
        scratch_shapes=[pltpu.VMEM(matrix.shape, F32), pltpu.SemaphoreType.DMA],
        input_output_aliases={3: 0, 4: 1, 5: 2},
        compiler_params=pltpu.CompilerParams(vmem_limit_bytes=24 * 1024 * 1024),
        name="reflect",
    )

    def one(step, carry):
        recv, vecs, images, marks = carry
        vecs, images, marks, send = advance(
            jnp.reshape(step, (1,)).astype(jnp.int32), recv, panel, vecs, images, marks, matrix
        )
        recv = lax.all_to_all(send, ("row", "col"), 0, 0, tiled=True)
        return recv.reshape(row_count, col_count, height), vecs, images, marks

    start = (
        jnp.zeros((row_count, col_count, height), F32),
        jnp.zeros(state.shape, F32),
        jnp.zeros(state.shape, F32),
        jnp.zeros(marks_shape.shape, F32),
    )
    recv, vecs, images, marks = lax.fori_loop(0, PB, one, start)

    where = jnp.stack([row_id, col_id]).astype(jnp.int32)
    updated = pl.pallas_call(
        last_body,
        out_shape=jax.ShapeDtypeStruct((height, width), F32),
        in_specs=[pl.BlockSpec(memory_space=pltpu.SMEM)] + [vmem() for _ in range(5)],
        out_specs=vmem(),
        scratch_shapes=[pltpu.VMEM(state.shape, F32), pltpu.VMEM(state.shape, F32)],
        compiler_params=pltpu.CompilerParams(vmem_limit_bytes=24 * 1024 * 1024),
        name="update",
    )(where, recv, vecs, images, marks, reduced[:height])

    psi_rows = lax.all_gather(psi, "col", axis=0, tiled=True)
    turn = lax.all_gather(eigvec.reshape(row_tiles, tile_size, width), "row", axis=1)
    rotated = jnp.dot(psi_rows, turn.reshape(bands, width), preferred_element_type=F32)
    tile_shape = (row_tiles, 1, tile_size, col_tiles, 1, tile_size)
    return (
        reduced[height:].reshape(tile_shape),
        updated.reshape(tile_shape),
        marks[0, :PB],
        marks[1, :PB],
        rotated.astype(jnp.bfloat16).reshape(g_rows * col_count, col_tiles, 1, tile_size),
    )


def solution(mesh):
    return jax.shard_map(
        on_device,
        mesh=mesh,
        in_specs=(
            P(("row", "col"), None),
            P(("row", "col"), None),
            P(None, "row", None, None, "col", None),
        ),
        out_specs=(
            P(None, "row", None, None, "col", None),
            P(None, "row", None, None, "col", None),
            P(),
            P(),
            P("row", None, "col", None),
        ),
        check_vma=False,
    )
```

```python
import functools

import jax
import jax.numpy as jnp
from jax import lax
from jax.experimental import pallas as pl
from jax.experimental.pallas import tpu as pltpu
from jax.sharding import PartitionSpec as P

PB = 16
LANES = 128
F32 = jnp.float32
MIB = 1024 * 1024


def total(x):
    return jnp.sum(jnp.sum(x, axis=-2, keepdims=True), axis=-1, keepdims=True)


def over_k(left, right):
    return lax.dot_general(left, right, (((1,), (0,)), ((), ())), preferred_element_type=F32)


def products_body(where_ref, *refs, row_tiles, col_tiles, gvecs):
    rows = refs[:row_tiles]
    head_ref = refs[row_tiles]
    cols = refs[row_tiles + 1 : row_tiles + 1 + col_tiles]
    blocks_out, strip_out, send_out, left_vmem, left_psi_vmem = refs[row_tiles + 1 + col_tiles :]
    height = row_tiles * LANES

    def swapped(x):
        return jnp.concatenate([x[:, 1:2], x[:, 0:1]], axis=1).reshape(-1, LANES)

    @pl.when(pl.program_id(0) == 0)
    def _():
        for k, ref in enumerate(rows):
            at = pl.ds(k * LANES, LANES)
            left_vmem[at, :] = swapped(ref[...]).T
            left_psi_vmem[at, :] = ref[:, 0].reshape(-1, LANES).T
        mine = jnp.concatenate([ref[...].reshape(-1, LANES) for ref in rows], axis=1)
        strip = 0.5 * over_k(swapped(head_ref[...]).T, mine)
        strip_out[...] = strip[:PB]
        send = jnp.concatenate([jnp.zeros((1, height), F32), strip[0:1]], axis=1)
        send_out[...] = jnp.broadcast_to(send[:, None, :], send_out.shape)

    both = jnp.concatenate([ref[...].reshape(-1, LANES) for ref in cols], axis=1)
    psi = jnp.concatenate([ref[:, 0].reshape(-1, LANES) for ref in cols], axis=1)
    blocks_out[0, :height, :] = 0.5 * over_k(left_vmem[...], both)
    blocks_out[0, height:, :] = over_k(left_psi_vmem[...], psi) * (1.0 / gvecs)


def gathered(recv_ref, at, counts, halves):
    row_count, col_count = counts
    parts = []
    for h in range(halves):
        start = at + h * LANES
        block = recv_ref[:, :, start : start + LANES].reshape(row_count, col_count, LANES)
        parts.append(jnp.sum(block, axis=1))
    return jnp.concatenate(parts, axis=0).reshape(1, row_count * halves, LANES)


def finish_image(image, vecs, images, vector, tau):
    along_w = total(images * vector)
    along_v = total(vecs * vector)
    image = image - jnp.sum(vecs * along_w + images * along_v, axis=0, keepdims=True)
    image = tau * image
    return image - 0.5 * tau * total(image * vector) * vector


def place(into, what, slot):
    slots = lax.broadcasted_iota(jnp.int32, (PB, 1, 1), 0)
    return jnp.where(slots == slot, what, into)


def step_body(
    step_ref, recv_ref, strip_ref, vecs_ref, images_ref, marks_ref, blocks_ref,
    vecs_out, images_out, marks_out, send_out, matrix_vmem, sem, *, counts,
):
    step = step_ref[0]
    tiles = vecs_ref.shape[1]
    col_count, height, width = matrix_vmem.shape
    halves = height // LANES
    copy = pltpu.make_async_copy(blocks_ref.at[:, :height, :], matrix_vmem, sem)
    copy.start()
    lane = lax.broadcasted_iota(jnp.int32, (1, 1, LANES), 2)
    marks = marks_ref[...]
    vecs = vecs_ref[...]
    images = images_ref[...]
    before = jnp.maximum(step - 1, 0)
    vector = vecs_ref[pl.ds(before, 1)]
    tau = marks[2:3, 0:1].reshape(1, 1, 1)
    image = finish_image(gathered(recv_ref, 0, counts, halves), vecs, images, vector, tau)
    images = place(images, image, step - 1)
    images_out[...] = images
    head_w = jnp.sum(jnp.where(lane == step, images[:, 0:1, :], 0.0), axis=-1, keepdims=True)
    head_v = jnp.sum(jnp.where(lane == step, vecs[:, 0:1, :], 0.0), axis=-1, keepdims=True)
    column = gathered(recv_ref, height, counts, halves) - jnp.sum(
        vecs * head_w + images * head_v, axis=0, keepdims=True
    )
    shape = (1, tiles, LANES)
    positions = lax.broadcasted_iota(jnp.int32, shape, 1) * LANES + lax.broadcasted_iota(
        jnp.int32, shape, 2
    )
    below = positions > step + 1
    pivot = total(jnp.where(positions == step + 1, column, 0.0))
    tail = total(jnp.where(below, column * column, 0.0))
    corner = total(jnp.where(positions == step, column, 0.0))
    length = jnp.sqrt(pivot * pivot + tail)
    beta = jnp.where(pivot >= 0.0, -length, length)
    tau = (beta - pivot) / beta
    vector = jnp.where(positions == step + 1, 1.0, jnp.where(below, column / (pivot - beta), 0.0))
    vecs_out[...] = place(vecs, vector, step)
    row = lax.broadcasted_iota(jnp.int32, marks.shape, 0)
    spot = lax.broadcasted_iota(jnp.int32, marks.shape, 1) == step
    flat = marks.shape
    marks = jnp.where((row == 0) & spot, jnp.broadcast_to(corner[0], flat), marks)
    marks = jnp.where((row == 1) & spot, jnp.broadcast_to(beta[0], flat), marks)
    marks_out[...] = jnp.where(row == 2, jnp.broadcast_to(tau[0], flat), marks)
    after = strip_ref[pl.ds(jnp.minimum(step + 1, PB - 1), 1), :]
    copy.wait()
    col_tiles = width // LANES
    sums = jnp.zeros((height, LANES), F32)
    for c in range(col_count):
        for a in range(col_tiles):
            u = a * col_count + c
            sums = sums + matrix_vmem[c, :, a * LANES : (a + 1) * LANES] * vector[0, u : u + 1, :]
    pieces = [
        jnp.sum(sums[k * LANES : (k + 1) * LANES].T, axis=0, keepdims=True) for k in range(halves)
    ]
    send = jnp.concatenate(pieces + [after], axis=1)
    send_out[...] = jnp.broadcast_to(send[:, None, :], send_out.shape)


def last_body(
    where_ref, recv_ref, vecs_ref, images_ref, marks_ref, tile_ref, psi_ref, turn_ref,
    updated_out, rotated_out, vecs_vmem, images_vmem, *, counts,
):
    rotated_out[...] = over_k(psi_ref[...], turn_ref[...]).astype(rotated_out.dtype)
    tiles = vecs_ref.shape[1]
    row_id = where_ref[0]
    col_id = where_ref[1]
    height, width = updated_out.shape
    row_tiles = height // LANES
    col_tiles = width // LANES
    vecs = vecs_ref[...]
    vector = vecs_ref[PB - 1 : PB]
    tau = marks_ref[2:3, 0:1].reshape(1, 1, 1)
    image = finish_image(gathered(recv_ref, 0, counts, row_tiles), vecs, images_ref[...], vector, tau)
    images_vmem[...] = place(images_ref[...], image, PB - 1)
    vecs_vmem[...] = vecs

    def part(ref, at):
        return ref[:, pl.ds(at, 1), :].reshape(PB, LANES)

    lefts = [
        jnp.concatenate([part(vecs_vmem, at), part(images_vmem, at)], axis=0)
        for at in (row_id + k * (tiles // row_tiles) for k in range(row_tiles))
    ]
    rights = [
        jnp.concatenate([part(images_vmem, at), part(vecs_vmem, at)], axis=0)
        for at in (col_id + k * (tiles // col_tiles) for k in range(col_tiles))
    ]
    left = jnp.concatenate(lefts, axis=1)
    right = jnp.concatenate(rights, axis=1)
    change = lax.dot_general(
        left, right, (((0,), (0,)), ((), ())),
        precision=lax.Precision.HIGHEST, preferred_element_type=F32,
    )
    updated_out[...] = tile_ref[0, :height, :] - change


def vmem():
    return pl.BlockSpec(memory_space=pltpu.VMEM)


def on_device(psi, hpsi, eigvec):
    g_rows, bands = psi.shape
    row_tiles, _, tile_size, col_tiles = eigvec.shape[:4]
    row_count = lax.axis_size("row")
    col_count = lax.axis_size("col")
    devices = row_count * col_count
    counts = (row_count, col_count)
    row_id = lax.axis_index("row")
    col_id = lax.axis_index("col")
    gvecs = g_rows * devices
    height = row_tiles * tile_size
    width = col_tiles * tile_size
    tiles = bands // tile_size
    where = jnp.stack([row_id, col_id]).astype(jnp.int32)

    both = lax.all_gather(jnp.stack([psi, hpsi]), "row")
    psi_rows = lax.all_gather(psi, "col", axis=0, tiled=True)
    turn = lax.all_gather(eigvec.reshape(row_tiles, tile_size, width), "row", axis=1)

    k = row_count * 2 * g_rows
    block = (row_count, 2, g_rows, tile_size)
    sent = jax.ShapeDtypeStruct((devices, 1, 2 * height), F32)

    def column_block(index):
        return pl.BlockSpec(block, lambda c, where: (0, 0, 0, index(c, where)))

    in_specs = (
        [column_block(lambda c, where, a=a: where[0] + a * row_count) for a in range(row_tiles)]
        + [column_block(lambda c, where: 0)]
        + [column_block(lambda c, where, a=a: c + a * col_count) for a in range(col_tiles)]
    )
    blocks, strip, send = pl.pallas_call(
        functools.partial(products_body, row_tiles=row_tiles, col_tiles=col_tiles, gvecs=gvecs),
        out_shape=(
            jax.ShapeDtypeStruct((col_count, 2 * height, width), F32),
            jax.ShapeDtypeStruct((PB, height), F32),
            sent,
        ),
        grid_spec=pltpu.PrefetchScalarGridSpec(
            num_scalar_prefetch=1,
            grid=(col_count,),
            in_specs=in_specs,
            out_specs=(
                pl.BlockSpec((1, 2 * height, width), lambda c, where: (c, 0, 0)),
                pl.BlockSpec((PB, height), lambda c, where: (0, 0)),
                pl.BlockSpec(sent.shape, lambda c, where: (0, 0, 0)),
            ),
            scratch_shapes=[
                pltpu.VMEM((height, k), psi.dtype),
                pltpu.VMEM((height, k // 2), psi.dtype),
            ],
        ),
        compiler_params=pltpu.CompilerParams(vmem_limit_bytes=32 * MIB),
        name="products",
    )(where, *([both] * len(in_specs)))

    reduced = lax.psum_scatter(blocks, "col", scatter_dimension=0, tiled=True)

    state = jax.ShapeDtypeStruct((PB, tiles, tile_size), F32)
    marks_shape = jax.ShapeDtypeStruct((8, tile_size), F32)
    advance = pl.pallas_call(
        functools.partial(step_body, counts=counts),
        out_shape=(state, state, marks_shape, sent),
        in_specs=[pl.BlockSpec(memory_space=pltpu.SMEM)]
        + [vmem() for _ in range(5)]
        + [pl.BlockSpec(memory_space=pltpu.HBM)],
        out_specs=tuple(vmem() for _ in range(4)),
        scratch_shapes=[
            pltpu.VMEM((col_count, height, width), F32),
            pltpu.SemaphoreType.DMA,
        ],
        input_output_aliases={3: 0, 4: 1, 5: 2},
        compiler_params=pltpu.CompilerParams(vmem_limit_bytes=24 * MIB),
        name="reflect",
    )

    def exchange(send):
        return lax.all_to_all(send, ("row", "col"), 0, 0, tiled=True)

    def one(step, carry):
        recv, vecs, images, marks = carry
        vecs, images, marks, send = advance(
            jnp.reshape(step, (1,)).astype(jnp.int32), recv, strip, vecs, images, marks, blocks
        )
        return exchange(send), vecs, images, marks

    start = (
        exchange(send),
        jnp.zeros(state.shape, F32),
        jnp.zeros(state.shape, F32),
        jnp.zeros(marks_shape.shape, F32),
    )
    recv, vecs, images, marks = lax.fori_loop(0, PB, one, start)

    updated, rotated = pl.pallas_call(
        functools.partial(last_body, counts=counts),
        out_shape=(
            jax.ShapeDtypeStruct((height, width), F32),
            jax.ShapeDtypeStruct((g_rows * col_count, width), psi.dtype),
        ),
        in_specs=[pl.BlockSpec(memory_space=pltpu.SMEM)] + [vmem() for _ in range(7)],
        out_specs=(vmem(), vmem()),
        scratch_shapes=[pltpu.VMEM(state.shape, F32), pltpu.VMEM(state.shape, F32)],
        compiler_params=pltpu.CompilerParams(vmem_limit_bytes=24 * MIB),
        name="update",
    )(where, recv, vecs, images, marks, reduced, psi_rows, turn.reshape(bands, width))

    tile_shape = (row_tiles, 1, tile_size, col_tiles, 1, tile_size)
    return (
        reduced[0, height:].reshape(tile_shape),
        updated.reshape(tile_shape),
        marks[0, :PB],
        marks[1, :PB],
        rotated.reshape(g_rows * col_count, col_tiles, 1, tile_size),
    )


def solution(mesh):
    return jax.shard_map(
        on_device,
        mesh=mesh,
        in_specs=(
            P(("row", "col"), None),
            P(("row", "col"), None),
            P(None, "row", None, None, "col", None),
        ),
        out_specs=(
            P(None, "row", None, None, "col", None),
            P(None, "row", None, None, "col", None),
            P(),
            P(),
            P("row", None, "col", None),
        ),
        check_vma=False,
    )
```

```python
import functools

import jax
import jax.numpy as jnp
from jax import lax
from jax.experimental import pallas as pl
from jax.experimental.pallas import tpu as pltpu
from jax.sharding import PartitionSpec as P

PB = 16
WIDE = 5
LANES = 128
F32 = jnp.float32
MIB = 1024 * 1024


def total(x):
    return jnp.sum(jnp.sum(x, axis=-2, keepdims=True), axis=-1, keepdims=True)


def over_k(left, right):
    return lax.dot_general(left, right, (((1,), (0,)), ((), ())), preferred_element_type=F32)


def products_body(where_ref, *refs, row_tiles, col_tiles, gvecs):
    rows = refs[:row_tiles]
    head_ref = refs[row_tiles]
    cols = refs[row_tiles + 1 : row_tiles + 1 + col_tiles]
    matrix_out, overlap_out, strip_out, left_vmem, left_psi_vmem = refs[row_tiles + 1 + col_tiles :]
    height = row_tiles * LANES

    def swapped(x):
        return jnp.concatenate([x[:, 1:2], x[:, 0:1]], axis=1).reshape(-1, LANES)

    @pl.when(pl.program_id(0) == 0)
    def _():
        for k, ref in enumerate(rows):
            at = pl.ds(k * LANES, LANES)
            left_vmem[at, :] = swapped(ref[...]).T
            left_psi_vmem[at, :] = ref[:, 0].reshape(-1, LANES).T
        left_vmem[height:, :] = swapped(head_ref[...]).T[:PB]

    both = jnp.concatenate([ref[...].reshape(-1, LANES) for ref in cols], axis=1)
    psi = jnp.concatenate([ref[:, 0].reshape(-1, LANES) for ref in cols], axis=1)
    mixed = 0.5 * over_k(left_vmem[...], both)
    matrix_out[0] = mixed[:height]
    strip_out[0] = mixed[height:]
    overlap_out[0] = over_k(left_psi_vmem[...], psi) * (1.0 / gvecs)


def gathered(recv_ref, row_count):
    recv = recv_ref[...]
    count = recv.shape[0] // row_count
    if count > 1:
        recv = jnp.sum(recv.reshape(row_count, count, *recv.shape[1:]), axis=1)
    return recv.reshape(1, -1, LANES)


def finish_image(image, vecs, images, vector, tau):
    along_w = total(images * vector)
    along_v = total(vecs * vector)
    image = image - jnp.sum(vecs * along_w + images * along_v, axis=0, keepdims=True)
    image = tau * image
    return image - 0.5 * tau * total(image * vector) * vector


def place(into, what, slot):
    slots = lax.broadcasted_iota(jnp.int32, (PB, 1, 1), 0)
    return jnp.where(slots == slot, what, into)


def spot_of(tile, row_count, row_tiles):
    return (tile % row_count) * row_tiles + tile // row_count


def step_body(
    step_ref, recv_ref, panel_ref, vecs_ref, images_ref, marks_ref, matrix_ref,
    vecs_out, images_out, marks_out, send_out, matrix_vmem, sem, *, row_count,
):
    step = step_ref[0]
    tiles = vecs_ref.shape[1]
    col_count, height, width = matrix_ref.shape
    copy = pltpu.make_async_copy(matrix_ref, matrix_vmem, sem)
    copy.start()
    row_tiles = height // LANES
    col_tiles = width // LANES
    lane = lax.broadcasted_iota(jnp.int32, (1, 1, LANES), 2)
    marks = marks_ref[...]
    vecs = vecs_ref[...]
    images = images_ref[...]
    before = jnp.maximum(step - 1, 0)
    vector = vecs_ref[pl.ds(before, 1)]
    tau = marks[2:3, 0:1].reshape(1, 1, 1)
    image = finish_image(gathered(recv_ref, row_count), vecs, images, vector, tau)
    images = place(images, image, step - 1)
    images_out[...] = images
    head_w = jnp.sum(jnp.where(lane == step, images[:, 0:1, :], 0.0), axis=-1, keepdims=True)
    head_v = jnp.sum(jnp.where(lane == step, vecs[:, 0:1, :], 0.0), axis=-1, keepdims=True)
    column = panel_ref[pl.ds(step, 1)] - jnp.sum(
        vecs * head_w + images * head_v, axis=0, keepdims=True
    )
    shape = (1, tiles, LANES)
    spot = lax.broadcasted_iota(jnp.int32, shape, 1)
    tile = lax.div(spot, row_tiles) + lax.rem(spot, row_tiles) * row_count
    positions = tile * LANES + lax.broadcasted_iota(jnp.int32, shape, 2)
    below = positions > step + 1
    pivot = total(jnp.where(positions == step + 1, column, 0.0))
    tail = total(jnp.where(below, column * column, 0.0))
    corner = total(jnp.where(positions == step, column, 0.0))
    length = jnp.sqrt(pivot * pivot + tail)
    beta = jnp.where(pivot >= 0.0, -length, length)
    tau = (beta - pivot) / beta
    vector = jnp.where(positions == step + 1, 1.0, jnp.where(below, column / (pivot - beta), 0.0))
    vecs_out[...] = place(vecs, vector, step)
    row = lax.broadcasted_iota(jnp.int32, marks.shape, 0)
    mark = lax.broadcasted_iota(jnp.int32, marks.shape, 1) == step
    flat = marks.shape
    marks = jnp.where((row == 0) & mark, jnp.broadcast_to(corner[0], flat), marks)
    marks = jnp.where((row == 1) & mark, jnp.broadcast_to(beta[0], flat), marks)
    marks_out[...] = jnp.where(row == 2, jnp.broadcast_to(tau[0], flat), marks)
    copy.wait()
    sums = jnp.zeros((height, LANES), F32)
    for c in range(col_count):
        for a in range(col_tiles):
            at = spot_of(a * col_count + c, row_count, row_tiles)
            sums = sums + matrix_vmem[c, :, a * LANES : (a + 1) * LANES] * vector[0, at : at + 1, :]
    send = jnp.concatenate(
        [
            jnp.sum(sums[k * LANES : (k + 1) * LANES].T, axis=0, keepdims=True)
            for k in range(row_tiles)
        ],
        axis=0,
    )
    send_out[...] = jnp.broadcast_to(send[None], send_out.shape)


def last_body(
    where_ref, recv_ref, vecs_ref, images_ref, marks_ref, matrix_ref, psi_ref, turn_ref,
    updated_out, rotated_out, tile_vmem, vecs_vmem, images_vmem, sem, *, row_count,
):
    row_id = where_ref[0]
    col_id = where_ref[1]
    copy = pltpu.make_async_copy(matrix_ref.at[col_id], tile_vmem, sem)
    copy.start()
    rotated_out[...] = over_k(psi_ref[...], turn_ref[...]).astype(rotated_out.dtype)
    height, width = updated_out.shape
    row_tiles = height // LANES
    col_tiles = width // LANES
    col_count = matrix_ref.shape[0]
    vecs = vecs_ref[...]
    vector = vecs_ref[PB - 1 : PB]
    tau = marks_ref[2:3, 0:1].reshape(1, 1, 1)
    image = finish_image(gathered(recv_ref, row_count), vecs, images_ref[...], vector, tau)
    images_vmem[...] = place(images_ref[...], image, PB - 1)
    vecs_vmem[...] = vecs

    def part(ref, tile):
        at = lax.rem(tile, row_count) * row_tiles + lax.div(tile, row_count)
        return ref[:, pl.ds(at, 1), :].reshape(PB, LANES)

    lefts = [
        jnp.concatenate([part(vecs_vmem, at), part(images_vmem, at)], axis=0)
        for at in (row_id + k * row_count for k in range(row_tiles))
    ]
    rights = [
        jnp.concatenate([part(images_vmem, at), part(vecs_vmem, at)], axis=0)
        for at in (col_id + k * col_count for k in range(col_tiles))
    ]
    left = jnp.concatenate(lefts, axis=1)
    right = jnp.concatenate(rights, axis=1)
    change = lax.dot_general(
        left, right, (((0,), (0,)), ((), ())),
        precision=lax.Precision.HIGHEST, preferred_element_type=F32,
    )
    copy.wait()
    updated_out[...] = tile_vmem[...] - change


def vmem():
    return pl.BlockSpec(memory_space=pltpu.VMEM)


def on_device(psi, hpsi, eigvec):
    g_rows, bands = psi.shape
    row_tiles, _, tile_size, col_tiles = eigvec.shape[:4]
    row_count = lax.axis_size("row")
    col_count = lax.axis_size("col")
    devices = row_count * col_count
    row_id = lax.axis_index("row")
    col_id = lax.axis_index("col")
    gvecs = g_rows * devices
    height = row_tiles * tile_size
    width = col_tiles * tile_size
    tiles = bands // tile_size
    where = jnp.stack([row_id, col_id]).astype(jnp.int32)

    both = lax.all_gather(jnp.stack([psi, hpsi]), "row")
    psi_rows = lax.all_to_all(
        jnp.broadcast_to(psi[None], (col_count, *psi.shape)), "col", 0, 0, tiled=True
    ).reshape(g_rows * col_count, bands)
    both, psi_rows = lax.optimization_barrier((both, psi_rows))

    k = row_count * 2 * g_rows
    block = (row_count, 2, g_rows, tile_size)

    def column_block(index):
        return pl.BlockSpec(block, lambda c, where: (0, 0, 0, index(c, where)))

    in_specs = (
        [column_block(lambda c, where, a=a: where[0] + a * row_count) for a in range(row_tiles)]
        + [column_block(lambda c, where: 0)]
        + [column_block(lambda c, where, a=a: c + a * col_count) for a in range(col_tiles)]
    )
    blocks_shape = jax.ShapeDtypeStruct((col_count, height, width), F32)
    strip_shape = jax.ShapeDtypeStruct((col_count, PB, width), F32)
    matrix, overlap, strip = pl.pallas_call(
        functools.partial(products_body, row_tiles=row_tiles, col_tiles=col_tiles, gvecs=gvecs),
        out_shape=(blocks_shape, blocks_shape, strip_shape),
        grid_spec=pltpu.PrefetchScalarGridSpec(
            num_scalar_prefetch=1,
            grid=(col_count,),
            in_specs=in_specs,
            out_specs=tuple(
                pl.BlockSpec((1, *made.shape[1:]), lambda c, where: (c, 0, 0))
                for made in (blocks_shape, blocks_shape, strip_shape)
            ),
            scratch_shapes=[
                pltpu.VMEM((height + PB, k), psi.dtype),
                pltpu.VMEM((height, k // 2), psi.dtype),
            ],
        ),
        compiler_params=pltpu.CompilerParams(vmem_limit_bytes=32 * MIB),
        name="products",
    )(where, *([both] * len(in_specs)))

    summed = lax.psum(matrix, "col")
    strip = jnp.sum(lax.all_to_all(strip, "col", 0, 0, tiled=True), axis=0)
    strip = lax.all_to_all(
        jnp.broadcast_to(strip[None], strip_shape.shape), "col", 0, 0, tiled=True
    )
    eigvec, overlap, strip = lax.optimization_barrier((eigvec, overlap, strip))
    panel = jnp.transpose(
        strip.reshape(col_count, PB, row_tiles, col_tiles // row_tiles, tile_size), (1, 3, 0, 2, 4)
    ).reshape(PB, tiles, tile_size)
    turn = lax.all_gather(eigvec.reshape(row_tiles, tile_size, width), "row", axis=1)
    correlation = lax.psum_scatter(overlap, "col", scatter_dimension=0, tiled=True)

    state = jax.ShapeDtypeStruct((PB, tiles, tile_size), F32)
    marks_shape = jax.ShapeDtypeStruct((8, tile_size), F32)

    def advance(peers, step, recv, vecs, images, marks, factor):
        return pl.pallas_call(
            functools.partial(step_body, row_count=row_count),
            out_shape=(
                state, state, marks_shape,
                jax.ShapeDtypeStruct((peers, row_tiles, tile_size), F32),
            ),
            in_specs=[pl.BlockSpec(memory_space=pltpu.SMEM)]
            + [vmem() for _ in range(5)]
            + [pl.BlockSpec(memory_space=pltpu.HBM)],
            out_specs=tuple(vmem() for _ in range(4)),
            scratch_shapes=[pltpu.VMEM(factor.shape, F32), pltpu.SemaphoreType.DMA],
            input_output_aliases={3: 0, 4: 1, 5: 2},
            compiler_params=pltpu.CompilerParams(vmem_limit_bytes=24 * MIB),
            name="reflect",
        )(jnp.reshape(step, (1,)).astype(jnp.int32), recv, panel, vecs, images, marks, factor)

    def wide(step, carry):
        vecs, images, marks, send = advance(devices, step, *carry, matrix)
        return lax.all_to_all(send, ("row", "col"), 0, 0, tiled=True), vecs, images, marks

    def narrow(step, carry):
        vecs, images, marks, send = advance(row_count, step, *carry, summed)
        return lax.all_to_all(send, "row", 0, 0, tiled=True), vecs, images, marks

    carry = (
        jnp.zeros((devices, row_tiles, tile_size), F32),
        jnp.zeros(state.shape, F32),
        jnp.zeros(state.shape, F32),
        jnp.zeros(marks_shape.shape, F32),
    )
    carry = lax.fori_loop(0, WIDE, wide, carry)
    carry = narrow(jnp.int32(WIDE), carry)
    recv, vecs, images, marks = lax.fori_loop(WIDE + 1, PB, narrow, carry)

    updated, rotated = pl.pallas_call(
        functools.partial(last_body, row_count=row_count),
        out_shape=(
            jax.ShapeDtypeStruct((height, width), F32),
            jax.ShapeDtypeStruct((g_rows * col_count, width), psi.dtype),
        ),
        in_specs=[pl.BlockSpec(memory_space=pltpu.SMEM)]
        + [vmem() for _ in range(4)]
        + [pl.BlockSpec(memory_space=pltpu.HBM), vmem(), vmem()],
        out_specs=(vmem(), vmem()),
        scratch_shapes=[
            pltpu.VMEM((height, width), F32),
            pltpu.VMEM(state.shape, F32),
            pltpu.VMEM(state.shape, F32),
            pltpu.SemaphoreType.DMA,
        ],
        compiler_params=pltpu.CompilerParams(vmem_limit_bytes=24 * MIB),
        name="update",
    )(where, recv, vecs, images, marks, summed, psi_rows, turn.reshape(bands, width))

    tile_shape = (row_tiles, 1, tile_size, col_tiles, 1, tile_size)
    return (
        correlation.reshape(tile_shape),
        updated.reshape(tile_shape),
        marks[0, :PB],
        marks[1, :PB],
        rotated.reshape(g_rows * col_count, col_tiles, 1, tile_size),
    )


def solution(mesh):
    return jax.shard_map(
        on_device,
        mesh=mesh,
        in_specs=(
            P(("row", "col"), None),
            P(("row", "col"), None),
            P(None, "row", None, None, "col", None),
        ),
        out_specs=(
            P(None, "row", None, None, "col", None),
            P(None, "row", None, None, "col", None),
            P(),
            P(),
            P("row", None, "col", None),
        ),
        check_vma=False,
    )
```

```python
import functools

import jax
import jax.numpy as jnp
from jax import lax
from jax.experimental import pallas as pl
from jax.experimental.pallas import tpu as pltpu
from jax.sharding import PartitionSpec as P

PB = 16
WIDE = 2
LANES = 128
F32 = jnp.float32
MIB = 1024 * 1024


def total(x):
    return jnp.sum(jnp.sum(x, axis=-2, keepdims=True), axis=-1, keepdims=True)


def over_k(left, right):
    return lax.dot_general(left, right, (((1,), (0,)), ((), ())), preferred_element_type=F32)


def products_body(where_ref, *refs, row_tiles, col_tiles, gvecs):
    rows = refs[:row_tiles]
    head_ref = refs[row_tiles]
    cols = refs[row_tiles + 1 : row_tiles + 1 + col_tiles]
    matrix_out, overlap_out, strip_out, left_vmem, left_psi_vmem = refs[row_tiles + 1 + col_tiles :]
    height = row_tiles * LANES

    def swapped(x):
        return jnp.concatenate([x[:, 1:2], x[:, 0:1]], axis=1).reshape(-1, LANES)

    @pl.when(pl.program_id(0) == 0)
    def _():
        for k, ref in enumerate(rows):
            at = pl.ds(k * LANES, LANES)
            left_vmem[at, :] = swapped(ref[...]).T
            left_psi_vmem[at, :] = ref[:, 0].reshape(-1, LANES).T
        left_vmem[height:, :] = swapped(head_ref[...]).T[:PB]

    both = jnp.concatenate([ref[...].reshape(-1, LANES) for ref in cols], axis=1)
    psi = jnp.concatenate([ref[:, 0].reshape(-1, LANES) for ref in cols], axis=1)
    mixed = 0.5 * over_k(left_vmem[...], both)
    matrix_out[0] = mixed[:height]
    strip_out[0] = mixed[height:]
    overlap_out[0] = over_k(left_psi_vmem[...], psi) * (1.0 / gvecs)


def gathered(recv_ref, row_count):
    recv = recv_ref[...]
    count = recv.shape[0] // row_count
    if count > 1:
        recv = jnp.sum(recv.reshape(row_count, count, *recv.shape[1:]), axis=1)
    return recv.reshape(1, -1, LANES)


def finish_image(image, vecs, images, vector, tau):
    along_w = total(images * vector)
    along_v = total(vecs * vector)
    image = image - jnp.sum(vecs * along_w + images * along_v, axis=0, keepdims=True)
    image = tau * image
    return image - 0.5 * tau * total(image * vector) * vector


def place(into, what, slot):
    slots = lax.broadcasted_iota(jnp.int32, (PB, 1, 1), 0)
    return jnp.where(slots == slot, what, into)


def spot_of(tile, row_count, row_tiles):
    return (tile % row_count) * row_tiles + tile // row_count


def step_body(
    step_ref, recv_ref, panel_ref, vecs_ref, images_ref, marks_ref, matrix_ref,
    vecs_out, images_out, marks_out, send_out, *, row_count,
):
    step = step_ref[0]
    tiles = vecs_ref.shape[1]
    col_count, height, width = matrix_ref.shape
    row_tiles = height // LANES
    col_tiles = width // LANES
    lane = lax.broadcasted_iota(jnp.int32, (1, 1, LANES), 2)
    marks = marks_ref[...]
    vecs = vecs_ref[...]
    images = images_ref[...]
    before = jnp.maximum(step - 1, 0)
    vector = vecs_ref[pl.ds(before, 1)]
    tau = marks[2:3, 0:1].reshape(1, 1, 1)
    image = finish_image(gathered(recv_ref, row_count), vecs, images, vector, tau)
    images = place(images, image, step - 1)
    images_out[...] = images
    head_w = jnp.sum(jnp.where(lane == step, images[:, 0:1, :], 0.0), axis=-1, keepdims=True)
    head_v = jnp.sum(jnp.where(lane == step, vecs[:, 0:1, :], 0.0), axis=-1, keepdims=True)
    column = panel_ref[pl.ds(step, 1)] - jnp.sum(
        vecs * head_w + images * head_v, axis=0, keepdims=True
    )
    shape = (1, tiles, LANES)
    spot = lax.broadcasted_iota(jnp.int32, shape, 1)
    tile = lax.div(spot, row_tiles) + lax.rem(spot, row_tiles) * row_count
    positions = tile * LANES + lax.broadcasted_iota(jnp.int32, shape, 2)
    below = positions > step + 1
    pivot = total(jnp.where(positions == step + 1, column, 0.0))
    tail = total(jnp.where(below, column * column, 0.0))
    corner = total(jnp.where(positions == step, column, 0.0))
    length = jnp.sqrt(pivot * pivot + tail)
    beta = jnp.where(pivot >= 0.0, -length, length)
    tau = (beta - pivot) / beta
    vector = jnp.where(positions == step + 1, 1.0, jnp.where(below, column / (pivot - beta), 0.0))
    vecs_out[...] = place(vecs, vector, step)
    row = lax.broadcasted_iota(jnp.int32, marks.shape, 0)
    mark = lax.broadcasted_iota(jnp.int32, marks.shape, 1) == step
    flat = marks.shape
    marks = jnp.where((row == 0) & mark, jnp.broadcast_to(corner[0], flat), marks)
    marks = jnp.where((row == 1) & mark, jnp.broadcast_to(beta[0], flat), marks)
    marks_out[...] = jnp.where(row == 2, jnp.broadcast_to(tau[0], flat), marks)
    sums = jnp.zeros((height, LANES), F32)
    for c in range(col_count):
        for a in range(col_tiles):
            at = spot_of(a * col_count + c, row_count, row_tiles)
            sums = sums + matrix_ref[c, :, a * LANES : (a + 1) * LANES] * vector[0, at : at + 1, :]
    send = jnp.concatenate(
        [
            jnp.sum(sums[k * LANES : (k + 1) * LANES].T, axis=0, keepdims=True)
            for k in range(row_tiles)
        ],
        axis=0,
    )
    send_out[...] = jnp.broadcast_to(send[None], send_out.shape)


def last_body(
    where_ref, recv_ref, vecs_ref, images_ref, marks_ref, matrix_ref, psi_ref, turn_ref,
    updated_out, rotated_out, tile_vmem, vecs_vmem, images_vmem, sem, *, row_count,
):
    row_id = where_ref[0]
    col_id = where_ref[1]
    copy = pltpu.make_async_copy(matrix_ref.at[col_id], tile_vmem, sem)
    copy.start()
    rotated_out[...] = over_k(psi_ref[...], turn_ref[...]).astype(rotated_out.dtype)
    height, width = updated_out.shape
    row_tiles = height // LANES
    col_tiles = width // LANES
    col_count = matrix_ref.shape[0]
    vecs = vecs_ref[...]
    vector = vecs_ref[PB - 1 : PB]
    tau = marks_ref[2:3, 0:1].reshape(1, 1, 1)
    image = finish_image(gathered(recv_ref, row_count), vecs, images_ref[...], vector, tau)
    images_vmem[...] = place(images_ref[...], image, PB - 1)
    vecs_vmem[...] = vecs

    def part(ref, tile):
        at = lax.rem(tile, row_count) * row_tiles + lax.div(tile, row_count)
        return ref[:, pl.ds(at, 1), :].reshape(PB, LANES)

    lefts = [
        jnp.concatenate([part(vecs_vmem, at), part(images_vmem, at)], axis=0)
        for at in (row_id + k * row_count for k in range(row_tiles))
    ]
    rights = [
        jnp.concatenate([part(images_vmem, at), part(vecs_vmem, at)], axis=0)
        for at in (col_id + k * col_count for k in range(col_tiles))
    ]
    left = jnp.concatenate(lefts, axis=1)
    right = jnp.concatenate(rights, axis=1)
    change = lax.dot_general(
        left, right, (((0,), (0,)), ((), ())),
        precision=lax.Precision.HIGHEST, preferred_element_type=F32,
    )
    copy.wait()
    updated_out[...] = tile_vmem[...] - change


def vmem():
    return pl.BlockSpec(memory_space=pltpu.VMEM)


def on_device(psi, hpsi, eigvec):
    g_rows, bands = psi.shape
    row_tiles, _, tile_size, col_tiles = eigvec.shape[:4]
    row_count = lax.axis_size("row")
    col_count = lax.axis_size("col")
    devices = row_count * col_count
    row_id = lax.axis_index("row")
    col_id = lax.axis_index("col")
    gvecs = g_rows * devices
    height = row_tiles * tile_size
    width = col_tiles * tile_size
    tiles = bands // tile_size
    where = jnp.stack([row_id, col_id]).astype(jnp.int32)

    both = lax.all_gather(jnp.stack([psi, hpsi]), "row")

    k = row_count * 2 * g_rows
    block = (row_count, 2, g_rows, tile_size)

    def column_block(index):
        return pl.BlockSpec(block, lambda c, where: (0, 0, 0, index(c, where)))

    in_specs = (
        [column_block(lambda c, where, a=a: where[0] + a * row_count) for a in range(row_tiles)]
        + [column_block(lambda c, where: 0)]
        + [column_block(lambda c, where, a=a: c + a * col_count) for a in range(col_tiles)]
    )
    blocks_shape = jax.ShapeDtypeStruct((col_count, height, width), F32)
    strip_shape = jax.ShapeDtypeStruct((col_count, PB, width), F32)
    matrix, overlap, strip = pl.pallas_call(
        functools.partial(products_body, row_tiles=row_tiles, col_tiles=col_tiles, gvecs=gvecs),
        out_shape=(blocks_shape, blocks_shape, strip_shape),
        grid_spec=pltpu.PrefetchScalarGridSpec(
            num_scalar_prefetch=1,
            grid=(col_count,),
            in_specs=in_specs,
            out_specs=tuple(
                pl.BlockSpec((1, *made.shape[1:]), lambda c, where: (c, 0, 0))
                for made in (blocks_shape, blocks_shape, strip_shape)
            ),
            scratch_shapes=[
                pltpu.VMEM((height + PB, k), psi.dtype),
                pltpu.VMEM((height, k // 2), psi.dtype),
            ],
        ),
        compiler_params=pltpu.CompilerParams(vmem_limit_bytes=60 * MIB),
        name="products",
    )(where, *([both] * len(in_specs)))

    summed = lax.psum(matrix, "col")
    strip = jnp.sum(lax.all_to_all(strip, "col", 0, 0, tiled=True), axis=0)
    strip = lax.all_to_all(
        jnp.broadcast_to(strip[None], strip_shape.shape), "col", 0, 0, tiled=True
    )
    eigvec, overlap, strip = lax.optimization_barrier((eigvec, overlap, strip))
    panel = jnp.transpose(
        strip.reshape(col_count, PB, row_tiles, col_tiles // row_tiles, tile_size), (1, 3, 0, 2, 4)
    ).reshape(PB, tiles, tile_size)
    turn = lax.all_gather(eigvec.reshape(row_tiles, tile_size, width), "row", axis=1)
    correlation = lax.psum_scatter(overlap, "col", scatter_dimension=0, tiled=True)

    state = jax.ShapeDtypeStruct((PB, tiles, tile_size), F32)
    marks_shape = jax.ShapeDtypeStruct((8, tile_size), F32)

    def advance(peers, step, recv, vecs, images, marks, factor):
        return pl.pallas_call(
            functools.partial(step_body, row_count=row_count),
            out_shape=(
                state, state, marks_shape,
                jax.ShapeDtypeStruct((peers, row_tiles, tile_size), F32),
            ),
            in_specs=[pl.BlockSpec(memory_space=pltpu.SMEM)]
            + [vmem() for _ in range(6)],
            out_specs=tuple(vmem() for _ in range(4)),
            input_output_aliases={3: 0, 4: 1, 5: 2},
            compiler_params=pltpu.CompilerParams(vmem_limit_bytes=24 * MIB),
            name="reflect",
        )(jnp.reshape(step, (1,)).astype(jnp.int32), recv, panel, vecs, images, marks, factor)

    def wide(step, carry):
        vecs, images, marks, send = advance(devices, step, *carry, matrix)
        return lax.all_to_all(send, ("row", "col"), 0, 0, tiled=True), vecs, images, marks

    def narrow(step, carry):
        vecs, images, marks, send = advance(row_count, step, *carry, summed)
        return lax.all_to_all(send, "row", 0, 0, tiled=True), vecs, images, marks

    carry = (
        jnp.zeros((devices, row_tiles, tile_size), F32),
        jnp.zeros(state.shape, F32),
        jnp.zeros(state.shape, F32),
        jnp.zeros(marks_shape.shape, F32),
    )
    carry = lax.fori_loop(0, WIDE, wide, carry)
    psi, carry = lax.optimization_barrier((psi, carry))
    psi_rows = lax.all_gather(psi, "col", axis=0, tiled=True)
    for step in range(WIDE, PB):
        carry = narrow(jnp.int32(step), carry)
    recv, vecs, images, marks = carry

    updated, rotated = pl.pallas_call(
        functools.partial(last_body, row_count=row_count),
        out_shape=(
            jax.ShapeDtypeStruct((height, width), F32),
            jax.ShapeDtypeStruct((g_rows * col_count, width), psi.dtype),
        ),
        in_specs=[pl.BlockSpec(memory_space=pltpu.SMEM)]
        + [vmem() for _ in range(4)]
        + [pl.BlockSpec(memory_space=pltpu.HBM), vmem(), vmem()],
        out_specs=(vmem(), vmem()),
        scratch_shapes=[
            pltpu.VMEM((height, width), F32),
            pltpu.VMEM(state.shape, F32),
            pltpu.VMEM(state.shape, F32),
            pltpu.SemaphoreType.DMA,
        ],
        compiler_params=pltpu.CompilerParams(vmem_limit_bytes=24 * MIB),
        name="update",
    )(where, recv, vecs, images, marks, summed, psi_rows, turn.reshape(bands, width))

    tile_shape = (row_tiles, 1, tile_size, col_tiles, 1, tile_size)
    return (
        correlation.reshape(tile_shape),
        updated.reshape(tile_shape),
        marks[0, :PB],
        marks[1, :PB],
        rotated.reshape(g_rows * col_count, col_tiles, 1, tile_size),
    )


def solution(mesh):
    return jax.shard_map(
        on_device,
        mesh=mesh,
        in_specs=(
            P(("row", "col"), None),
            P(("row", "col"), None),
            P(None, "row", None, None, "col", None),
        ),
        out_specs=(
            P(None, "row", None, None, "col", None),
            P(None, "row", None, None, "col", None),
            P(),
            P(),
            P("row", None, "col", None),
        ),
        check_vma=False,
    )
```

```python
import functools

import jax
import jax.numpy as jnp
from jax import lax
from jax.experimental import pallas as pl
from jax.experimental.pallas import tpu as pltpu
from jax.sharding import PartitionSpec as P

PB = 16
WIDE = 1
LANES = 128
F32 = jnp.float32
MIB = 1024 * 1024


def total(x):
    return jnp.sum(jnp.sum(x, axis=-2, keepdims=True), axis=-1, keepdims=True)


def over_k(left, right):
    return lax.dot_general(left, right, (((1,), (0,)), ((), ())), preferred_element_type=F32)


def products_body(where_ref, *refs, row_tiles, col_tiles, gvecs):
    rows = refs[:row_tiles]
    head_ref = refs[row_tiles]
    cols = refs[row_tiles + 1 : row_tiles + 1 + col_tiles]
    matrix_out, overlap_out, strip_out, left_vmem, left_psi_vmem = refs[row_tiles + 1 + col_tiles :]
    height = row_tiles * LANES

    def swapped(x):
        return jnp.concatenate([x[:, 1:2], x[:, 0:1]], axis=1).reshape(-1, LANES)

    @pl.when(pl.program_id(0) == 0)
    def _():
        for k, ref in enumerate(rows):
            at = pl.ds(k * LANES, LANES)
            left_vmem[at, :] = swapped(ref[...]).T
            left_psi_vmem[at, :] = ref[:, 0].reshape(-1, LANES).T
        left_vmem[height:, :] = swapped(head_ref[...]).T[:PB]

    both = jnp.concatenate([ref[...].reshape(-1, LANES) for ref in cols], axis=1)
    psi = jnp.concatenate([ref[:, 0].reshape(-1, LANES) for ref in cols], axis=1)
    mixed = 0.5 * over_k(left_vmem[...], both)
    matrix_out[0] = mixed[:height]
    strip_out[0] = mixed[height:]
    overlap_out[0] = over_k(left_psi_vmem[...], psi) * (1.0 / gvecs)


def gathered(recv_ref, row_count):
    recv = recv_ref[...]
    count = recv.shape[0] // row_count
    if count > 1:
        recv = jnp.sum(recv.reshape(row_count, count, *recv.shape[1:]), axis=1)
    return recv.reshape(1, -1, LANES)


def finish_image(image, vecs, images, vector, tau):
    along_w = total(images * vector)
    along_v = total(vecs * vector)
    image = image - jnp.sum(vecs * along_w + images * along_v, axis=0, keepdims=True)
    image = tau * image
    return image - 0.5 * tau * total(image * vector) * vector


def place(into, what, slot):
    slots = lax.broadcasted_iota(jnp.int32, (PB, 1, 1), 0)
    return jnp.where(slots == slot, what, into)


def spot_of(tile, row_count, row_tiles):
    return (tile % row_count) * row_tiles + tile // row_count


def step_body(
    step_ref, recv_ref, panel_ref, vecs_ref, images_ref, marks_ref, matrix_ref,
    vecs_out, images_out, marks_out, send_out, *, row_count,
):
    step = step_ref[0]
    tiles = vecs_ref.shape[1]
    col_count, height, width = matrix_ref.shape
    row_tiles = height // LANES
    col_tiles = width // LANES
    lane = lax.broadcasted_iota(jnp.int32, (1, 1, LANES), 2)
    marks = marks_ref[...]
    vecs = vecs_ref[...]
    images = images_ref[...]
    before = jnp.maximum(step - 1, 0)
    vector = vecs_ref[pl.ds(before, 1)]
    tau = marks[2:3, 0:1].reshape(1, 1, 1)
    image = finish_image(gathered(recv_ref, row_count), vecs, images, vector, tau)
    images = place(images, image, step - 1)
    images_out[...] = images
    head_w = jnp.sum(jnp.where(lane == step, images[:, 0:1, :], 0.0), axis=-1, keepdims=True)
    head_v = jnp.sum(jnp.where(lane == step, vecs[:, 0:1, :], 0.0), axis=-1, keepdims=True)
    column = panel_ref[pl.ds(step, 1)] - jnp.sum(
        vecs * head_w + images * head_v, axis=0, keepdims=True
    )
    shape = (1, tiles, LANES)
    spot = lax.broadcasted_iota(jnp.int32, shape, 1)
    tile = lax.div(spot, row_tiles) + lax.rem(spot, row_tiles) * row_count
    positions = tile * LANES + lax.broadcasted_iota(jnp.int32, shape, 2)
    below = positions > step + 1
    pivot = total(jnp.where(positions == step + 1, column, 0.0))
    tail = total(jnp.where(below, column * column, 0.0))
    corner = total(jnp.where(positions == step, column, 0.0))
    length = jnp.sqrt(pivot * pivot + tail)
    beta = jnp.where(pivot >= 0.0, -length, length)
    tau = (beta - pivot) / beta
    vector = jnp.where(positions == step + 1, 1.0, jnp.where(below, column / (pivot - beta), 0.0))
    vecs_out[...] = place(vecs, vector, step)
    row = lax.broadcasted_iota(jnp.int32, marks.shape, 0)
    mark = lax.broadcasted_iota(jnp.int32, marks.shape, 1) == step
    flat = marks.shape
    marks = jnp.where((row == 0) & mark, jnp.broadcast_to(corner[0], flat), marks)
    marks = jnp.where((row == 1) & mark, jnp.broadcast_to(beta[0], flat), marks)
    marks_out[...] = jnp.where(row == 2, jnp.broadcast_to(tau[0], flat), marks)
    sums = jnp.zeros((height, LANES), F32)
    for c in range(col_count):
        for a in range(col_tiles):
            at = spot_of(a * col_count + c, row_count, row_tiles)
            sums = sums + matrix_ref[c, :, a * LANES : (a + 1) * LANES] * vector[0, at : at + 1, :]
    send = jnp.concatenate(
        [
            jnp.sum(sums[k * LANES : (k + 1) * LANES].T, axis=0, keepdims=True)
            for k in range(row_tiles)
        ],
        axis=0,
    )
    send_out[...] = jnp.broadcast_to(send[None], send_out.shape)


def last_body(
    where_ref, recv_ref, vecs_ref, images_ref, marks_ref, tile_ref,
    updated_out, vecs_vmem, images_vmem, *, row_count, col_count,
):
    row_id = where_ref[0]
    col_id = where_ref[1]
    height, width = updated_out.shape
    row_tiles = height // LANES
    col_tiles = width // LANES
    vecs = vecs_ref[...]
    vector = vecs_ref[PB - 1 : PB]
    tau = marks_ref[2:3, 0:1].reshape(1, 1, 1)
    image = finish_image(gathered(recv_ref, row_count), vecs, images_ref[...], vector, tau)
    images_vmem[...] = place(images_ref[...], image, PB - 1)
    vecs_vmem[...] = vecs

    def part(ref, tile):
        at = lax.rem(tile, row_count) * row_tiles + lax.div(tile, row_count)
        return ref[:, pl.ds(at, 1), :].reshape(PB, LANES)

    lefts = [
        jnp.concatenate([part(vecs_vmem, at), part(images_vmem, at)], axis=0)
        for at in (row_id + k * row_count for k in range(row_tiles))
    ]
    rights = [
        jnp.concatenate([part(images_vmem, at), part(vecs_vmem, at)], axis=0)
        for at in (col_id + k * col_count for k in range(col_tiles))
    ]
    left = jnp.concatenate(lefts, axis=1)
    right = jnp.concatenate(rights, axis=1)
    change = lax.dot_general(
        left, right, (((0,), (0,)), ((), ())),
        precision=lax.Precision.HIGHEST, preferred_element_type=F32,
    )
    updated_out[...] = tile_ref[...] - change


def vmem():
    return pl.BlockSpec(memory_space=pltpu.VMEM)


def on_device(psi, hpsi, eigvec):
    g_rows, bands = psi.shape
    row_tiles, _, tile_size, col_tiles = eigvec.shape[:4]
    row_count = lax.axis_size("row")
    col_count = lax.axis_size("col")
    devices = row_count * col_count
    row_id = lax.axis_index("row")
    col_id = lax.axis_index("col")
    gvecs = g_rows * devices
    height = row_tiles * tile_size
    width = col_tiles * tile_size
    tiles = bands // tile_size
    where = jnp.stack([row_id, col_id]).astype(jnp.int32)

    both = lax.all_gather(jnp.stack([psi, hpsi]), "row")

    k = row_count * 2 * g_rows
    block = (row_count, 2, g_rows, tile_size)

    def column_block(index):
        return pl.BlockSpec(block, lambda c, where: (0, 0, 0, index(c, where)))

    in_specs = (
        [column_block(lambda c, where, a=a: where[0] + a * row_count) for a in range(row_tiles)]
        + [column_block(lambda c, where: 0)]
        + [column_block(lambda c, where, a=a: c + a * col_count) for a in range(col_tiles)]
    )
    blocks_shape = jax.ShapeDtypeStruct((col_count, height, width), F32)
    strip_shape = jax.ShapeDtypeStruct((col_count, PB, width), F32)
    matrix, overlap, strip = pl.pallas_call(
        functools.partial(products_body, row_tiles=row_tiles, col_tiles=col_tiles, gvecs=gvecs),
        out_shape=(blocks_shape, blocks_shape, strip_shape),
        grid_spec=pltpu.PrefetchScalarGridSpec(
            num_scalar_prefetch=1,
            grid=(col_count,),
            in_specs=in_specs,
            out_specs=tuple(
                pl.BlockSpec((1, *made.shape[1:]), lambda c, where: (c, 0, 0))
                for made in (blocks_shape, blocks_shape, strip_shape)
            ),
            scratch_shapes=[
                pltpu.VMEM((height + PB, k), psi.dtype),
                pltpu.VMEM((height, k // 2), psi.dtype),
            ],
        ),
        compiler_params=pltpu.CompilerParams(vmem_limit_bytes=60 * MIB),
        name="products",
    )(where, *([both] * len(in_specs)))

    summed = lax.psum(matrix, "col")
    strip = lax.all_to_all(strip, "col", 0, 0, tiled=True)
    strip = jnp.sum(strip, axis=0)
    strip = lax.all_to_all(
        jnp.broadcast_to(strip[None], strip_shape.shape), "col", 0, 0, tiled=True
    )
    panel = jnp.transpose(
        strip.reshape(col_count, PB, row_tiles, col_tiles // row_tiles, tile_size), (1, 3, 0, 2, 4)
    ).reshape(PB, tiles, tile_size)

    state = jax.ShapeDtypeStruct((PB, tiles, tile_size), F32)
    marks_shape = jax.ShapeDtypeStruct((8, tile_size), F32)

    def advance(peers, step, recv, vecs, images, marks, factor):
        return pl.pallas_call(
            functools.partial(step_body, row_count=row_count),
            out_shape=(
                state, state, marks_shape,
                jax.ShapeDtypeStruct((peers, row_tiles, tile_size), F32),
            ),
            in_specs=[pl.BlockSpec(memory_space=pltpu.SMEM)]
            + [vmem() for _ in range(6)],
            out_specs=tuple(vmem() for _ in range(4)),
            input_output_aliases={3: 0, 4: 1, 5: 2},
            compiler_params=pltpu.CompilerParams(vmem_limit_bytes=24 * MIB),
            name="reflect",
        )(jnp.reshape(step, (1,)).astype(jnp.int32), recv, panel, vecs, images, marks, factor)

    def wide(step, carry):
        vecs, images, marks, send = advance(devices, step, *carry, matrix)
        return lax.all_to_all(send, ("row", "col"), 0, 0, tiled=True), vecs, images, marks

    def narrow(step, carry):
        vecs, images, marks, send = advance(row_count, step, *carry, summed)
        return lax.all_to_all(send, "row", 0, 0, tiled=True), vecs, images, marks

    carry = (
        jnp.zeros((devices, row_tiles, tile_size), F32),
        jnp.zeros(state.shape, F32),
        jnp.zeros(state.shape, F32),
        jnp.zeros(marks_shape.shape, F32),
    )
    bound = jnp.where(row_id >= 0, jnp.int32(WIDE), jnp.int32(0))
    carry = lax.fori_loop(0, lax.optimization_barrier(bound), wide, carry)
    psi, eigvec, carry = lax.optimization_barrier((psi, eigvec, carry))
    psi_rows = lax.all_gather(psi, "col", axis=0, tiled=True)
    turn = lax.all_to_all(
        jnp.broadcast_to(
            eigvec.reshape(1, row_tiles, tile_size, width), (row_count, row_tiles, tile_size, width)
        ),
        "row", 0, 0, tiled=True,
    )
    turn, carry = lax.optimization_barrier((turn, carry))
    carry = narrow(jnp.int32(WIDE), carry)
    tile = lax.dynamic_index_in_dim(summed, col_id, 0, keepdims=False)
    overlap, carry = lax.optimization_barrier((overlap, carry))
    correlation = lax.psum_scatter(overlap, "col", scatter_dimension=0, tiled=True)
    for step in range(WIDE + 1, PB - 1):
        carry = narrow(jnp.int32(step), carry)
    psi_rows, turn, carry = lax.optimization_barrier((psi_rows, turn, carry))
    turn = jnp.transpose(turn, (1, 0, 2, 3)).reshape(bands, width)
    rotated = jnp.dot(psi_rows, turn, preferred_element_type=F32).astype(psi.dtype)
    recv, vecs, images, marks = narrow(jnp.int32(PB - 1), carry)

    updated = pl.pallas_call(
        functools.partial(last_body, row_count=row_count, col_count=col_count),
        out_shape=jax.ShapeDtypeStruct((height, width), F32),
        in_specs=[pl.BlockSpec(memory_space=pltpu.SMEM)]
        + [vmem() for _ in range(5)],
        out_specs=vmem(),
        scratch_shapes=[pltpu.VMEM(state.shape, F32), pltpu.VMEM(state.shape, F32)],
        compiler_params=pltpu.CompilerParams(vmem_limit_bytes=24 * MIB),
        name="update",
    )(where, recv, vecs, images, marks, tile)

    tile_shape = (row_tiles, 1, tile_size, col_tiles, 1, tile_size)
    return (
        correlation.reshape(tile_shape),
        updated.reshape(tile_shape),
        marks[0, :PB],
        marks[1, :PB],
        rotated.reshape(g_rows * col_count, col_tiles, 1, tile_size),
    )


def solution(mesh):
    return jax.shard_map(
        on_device,
        mesh=mesh,
        in_specs=(
            P(("row", "col"), None),
            P(("row", "col"), None),
            P(None, "row", None, None, "col", None),
        ),
        out_specs=(
            P(None, "row", None, None, "col", None),
            P(None, "row", None, None, "col", None),
            P(),
            P(),
            P("row", None, "col", None),
        ),
        check_vma=False,
    )
```

```python
import functools

import jax
import jax.numpy as jnp
from jax import lax
from jax.experimental import pallas as pl
from jax.experimental.pallas import tpu as pltpu
from jax.sharding import PartitionSpec as P

PB = 16
WIDE = 3
LANES = 128
F32 = jnp.float32
MIB = 1024 * 1024


def total(x):
    return jnp.sum(jnp.sum(x, axis=-2, keepdims=True), axis=-1, keepdims=True)


def over_k(left, right):
    return lax.dot_general(left, right, (((1,), (0,)), ((), ())), preferred_element_type=F32)


def products_body(where_ref, *refs, row_tiles, col_tiles, gvecs):
    rows = refs[:row_tiles]
    head_ref = refs[row_tiles]
    cols = refs[row_tiles + 1 : row_tiles + 1 + col_tiles]
    matrix_out, overlap_out, strip_out, left_vmem, left_psi_vmem = refs[row_tiles + 1 + col_tiles :]
    height = row_tiles * LANES

    def swapped(x):
        return jnp.concatenate([x[:, 1:2], x[:, 0:1]], axis=1).reshape(-1, LANES)

    @pl.when(pl.program_id(0) == 0)
    def _():
        for k, ref in enumerate(rows):
            at = pl.ds(k * LANES, LANES)
            left_vmem[at, :] = swapped(ref[...]).T
            left_psi_vmem[at, :] = ref[:, 0].reshape(-1, LANES).T
        left_vmem[height:, :] = swapped(head_ref[...]).T[:PB]

    both = jnp.concatenate([ref[...].reshape(-1, LANES) for ref in cols], axis=1)
    psi = jnp.concatenate([ref[:, 0].reshape(-1, LANES) for ref in cols], axis=1)
    mixed = 0.5 * over_k(left_vmem[...], both)
    matrix_out[0] = mixed[:height]
    strip_out[0] = mixed[height:]
    overlap_out[0] = over_k(left_psi_vmem[...], psi) * (1.0 / gvecs)


def gathered(recv_ref, row_count):
    recv = recv_ref[...]
    count = recv.shape[0] // row_count
    if count > 1:
        recv = jnp.sum(recv.reshape(row_count, count, *recv.shape[1:]), axis=1)
    return recv.reshape(1, -1, LANES)


def finish_image(image, vecs, images, vector, tau):
    along_w = total(images * vector)
    along_v = total(vecs * vector)
    image = image - jnp.sum(vecs * along_w + images * along_v, axis=0, keepdims=True)
    image = tau * image
    return image - 0.5 * tau * total(image * vector) * vector


def place(into, what, slot):
    slots = lax.broadcasted_iota(jnp.int32, (PB, 1, 1), 0)
    return jnp.where(slots == slot, what, into)


def spot_of(tile, row_count, row_tiles):
    return (tile % row_count) * row_tiles + tile // row_count


def step_body(
    step_ref, recv_ref, panel_ref, vecs_ref, images_ref, marks_ref, matrix_ref,
    vecs_out, images_out, marks_out, send_out, *, row_count,
):
    step = step_ref[0]
    tiles = vecs_ref.shape[1]
    col_count, height, width = matrix_ref.shape
    row_tiles = height // LANES
    col_tiles = width // LANES
    lane = lax.broadcasted_iota(jnp.int32, (1, 1, LANES), 2)
    marks = marks_ref[...]
    vecs = vecs_ref[...]
    images = images_ref[...]
    before = jnp.maximum(step - 1, 0)
    vector = vecs_ref[pl.ds(before, 1)]
    tau = marks[2:3, 0:1].reshape(1, 1, 1)
    image = finish_image(gathered(recv_ref, row_count), vecs, images, vector, tau)
    images = place(images, image, step - 1)
    images_out[...] = images
    head_w = jnp.sum(jnp.where(lane == step, images[:, 0:1, :], 0.0), axis=-1, keepdims=True)
    head_v = jnp.sum(jnp.where(lane == step, vecs[:, 0:1, :], 0.0), axis=-1, keepdims=True)
    column = panel_ref[pl.ds(step, 1)] - jnp.sum(
        vecs * head_w + images * head_v, axis=0, keepdims=True
    )
    shape = (1, tiles, LANES)
    spot = lax.broadcasted_iota(jnp.int32, shape, 1)
    tile = lax.div(spot, row_tiles) + lax.rem(spot, row_tiles) * row_count
    positions = tile * LANES + lax.broadcasted_iota(jnp.int32, shape, 2)
    below = positions > step + 1
    pivot = total(jnp.where(positions == step + 1, column, 0.0))
    tail = total(jnp.where(below, column * column, 0.0))
    corner = total(jnp.where(positions == step, column, 0.0))
    length = jnp.sqrt(pivot * pivot + tail)
    beta = jnp.where(pivot >= 0.0, -length, length)
    tau = (beta - pivot) / beta
    vector = jnp.where(positions == step + 1, 1.0, jnp.where(below, column / (pivot - beta), 0.0))
    vecs_out[...] = place(vecs, vector, step)
    row = lax.broadcasted_iota(jnp.int32, marks.shape, 0)
    mark = lax.broadcasted_iota(jnp.int32, marks.shape, 1) == step
    flat = marks.shape
    marks = jnp.where((row == 0) & mark, jnp.broadcast_to(corner[0], flat), marks)
    marks = jnp.where((row == 1) & mark, jnp.broadcast_to(beta[0], flat), marks)
    marks_out[...] = jnp.where(row == 2, jnp.broadcast_to(tau[0], flat), marks)
    sums = jnp.zeros((height, LANES), F32)
    for c in range(col_count):
        for a in range(col_tiles):
            at = spot_of(a * col_count + c, row_count, row_tiles)
            sums = sums + matrix_ref[c, :, a * LANES : (a + 1) * LANES] * vector[0, at : at + 1, :]
    send = jnp.concatenate(
        [
            jnp.sum(sums[k * LANES : (k + 1) * LANES].T, axis=0, keepdims=True)
            for k in range(row_tiles)
        ],
        axis=0,
    )
    send_out[...] = jnp.broadcast_to(send[None], send_out.shape)


def last_body(
    where_ref, recv_ref, vecs_ref, images_ref, marks_ref, tile_ref,
    updated_out, vecs_vmem, images_vmem, *, row_count, col_count,
):
    row_id = where_ref[0]
    col_id = where_ref[1]
    height, width = updated_out.shape
    row_tiles = height // LANES
    col_tiles = width // LANES
    vecs = vecs_ref[...]
    vector = vecs_ref[PB - 1 : PB]
    tau = marks_ref[2:3, 0:1].reshape(1, 1, 1)
    image = finish_image(gathered(recv_ref, row_count), vecs, images_ref[...], vector, tau)
    images_vmem[...] = place(images_ref[...], image, PB - 1)
    vecs_vmem[...] = vecs

    def part(ref, tile):
        at = lax.rem(tile, row_count) * row_tiles + lax.div(tile, row_count)
        return ref[:, pl.ds(at, 1), :].reshape(PB, LANES)

    lefts = [
        jnp.concatenate([part(vecs_vmem, at), part(images_vmem, at)], axis=0)
        for at in (row_id + k * row_count for k in range(row_tiles))
    ]
    rights = [
        jnp.concatenate([part(images_vmem, at), part(vecs_vmem, at)], axis=0)
        for at in (col_id + k * col_count for k in range(col_tiles))
    ]
    left = jnp.concatenate(lefts, axis=1)
    right = jnp.concatenate(rights, axis=1)
    change = lax.dot_general(
        left, right, (((0,), (0,)), ((), ())),
        precision=lax.Precision.HIGHEST, preferred_element_type=F32,
    )
    updated_out[...] = tile_ref[...] - change


def rotate_body(psi_ref, both_ref, rotated_out, *, row_tiles, tile_size):
    row_count, _, g_rows, bands = both_ref.shape
    width = rotated_out.shape[1]
    pieces = tile_size // g_rows
    sums = jnp.zeros(rotated_out.shape, F32)
    for a in range(row_tiles):
        for r in range(0, row_count, 2):
            turn = jnp.concatenate(
                [
                    both_ref[q, 0, :, (a * pieces + s) * width : (a * pieces + s + 1) * width]
                    for q in (r, r + 1)
                    for s in range(pieces)
                ],
                axis=0,
            )
            at = (a * row_count + r) * tile_size
            sums = sums + over_k(psi_ref[:, at : at + 2 * tile_size], turn)
    rotated_out[...] = sums.astype(rotated_out.dtype)


def vmem():
    return pl.BlockSpec(memory_space=pltpu.VMEM)


def on_device(psi, hpsi, eigvec):
    g_rows, bands = psi.shape
    row_tiles, _, tile_size, col_tiles = eigvec.shape[:4]
    row_count = lax.axis_size("row")
    col_count = lax.axis_size("col")
    devices = row_count * col_count
    row_id = lax.axis_index("row")
    col_id = lax.axis_index("col")
    gvecs = g_rows * devices
    height = row_tiles * tile_size
    width = col_tiles * tile_size
    tiles = bands // tile_size
    where = jnp.stack([row_id, col_id]).astype(jnp.int32)

    lanes = bands // width
    folded = jnp.transpose(eigvec.reshape(lanes, g_rows, width), (1, 0, 2)).reshape(g_rows, bands)
    both = lax.all_gather(jnp.stack([psi, hpsi, folded]), "row")

    k = row_count * 2 * g_rows
    block = (row_count, 2, g_rows, tile_size)

    def column_block(index):
        return pl.BlockSpec(block, lambda c, where: (0, 0, 0, index(c, where)))

    in_specs = (
        [column_block(lambda c, where, a=a: where[0] + a * row_count) for a in range(row_tiles)]
        + [column_block(lambda c, where: 0)]
        + [column_block(lambda c, where, a=a: c + a * col_count) for a in range(col_tiles)]
    )
    blocks_shape = jax.ShapeDtypeStruct((col_count, height, width), F32)
    strip_shape = jax.ShapeDtypeStruct((col_count, PB, width), F32)
    matrix, overlap, strip = pl.pallas_call(
        functools.partial(products_body, row_tiles=row_tiles, col_tiles=col_tiles, gvecs=gvecs),
        out_shape=(blocks_shape, blocks_shape, strip_shape),
        grid_spec=pltpu.PrefetchScalarGridSpec(
            num_scalar_prefetch=1,
            grid=(col_count,),
            in_specs=in_specs,
            out_specs=tuple(
                pl.BlockSpec((1, *made.shape[1:]), lambda c, where: (c, 0, 0))
                for made in (blocks_shape, blocks_shape, strip_shape)
            ),
            scratch_shapes=[
                pltpu.VMEM((height + PB, k), psi.dtype),
                pltpu.VMEM((height, k // 2), psi.dtype),
            ],
        ),
        compiler_params=pltpu.CompilerParams(vmem_limit_bytes=60 * MIB),
        name="products",
    )(where, *([both] * len(in_specs)))

    summed = lax.psum(matrix, "col")
    strip = lax.all_to_all(strip, "col", 0, 0, tiled=True)
    strip = jnp.sum(strip, axis=0)
    strip = lax.all_to_all(
        jnp.broadcast_to(strip[None], strip_shape.shape), "col", 0, 0, tiled=True
    )
    panel = jnp.transpose(
        strip.reshape(col_count, PB, row_tiles, col_tiles // row_tiles, tile_size), (1, 3, 0, 2, 4)
    ).reshape(PB, tiles, tile_size)

    state = jax.ShapeDtypeStruct((PB, tiles, tile_size), F32)
    marks_shape = jax.ShapeDtypeStruct((8, tile_size), F32)

    def advance(peers, step, recv, vecs, images, marks, factor):
        return pl.pallas_call(
            functools.partial(step_body, row_count=row_count),
            out_shape=(
                state, state, marks_shape,
                jax.ShapeDtypeStruct((peers, row_tiles, tile_size), F32),
            ),
            in_specs=[pl.BlockSpec(memory_space=pltpu.SMEM)]
            + [vmem() for _ in range(6)],
            out_specs=tuple(vmem() for _ in range(4)),
            input_output_aliases={3: 0, 4: 1, 5: 2},
            compiler_params=pltpu.CompilerParams(vmem_limit_bytes=24 * MIB),
            name="reflect",
        )(jnp.reshape(step, (1,)).astype(jnp.int32), recv, panel, vecs, images, marks, factor)

    def wide(step, carry):
        vecs, images, marks, send = advance(devices, step, *carry, matrix)
        return lax.all_to_all(send, ("row", "col"), 0, 0, tiled=True), vecs, images, marks

    def narrow(step, carry):
        vecs, images, marks, send = advance(row_count, step, *carry, summed)
        return lax.all_to_all(send, "row", 0, 0, tiled=True), vecs, images, marks

    carry = (
        jnp.zeros((devices, row_tiles, tile_size), F32),
        jnp.zeros(state.shape, F32),
        jnp.zeros(state.shape, F32),
        jnp.zeros(marks_shape.shape, F32),
    )
    carry = lax.fori_loop(0, WIDE, wide, carry)
    psi, carry = lax.optimization_barrier((psi, carry))
    psi_rows = lax.all_gather(psi, "col", axis=0, tiled=True)
    carry = narrow(jnp.int32(WIDE), carry)
    tile = lax.dynamic_index_in_dim(summed, col_id, 0, keepdims=False)
    overlap, carry = lax.optimization_barrier((overlap, carry))
    correlation = lax.psum_scatter(overlap, "col", scatter_dimension=0, tiled=True)
    for step in range(WIDE + 1, PB - 1):
        carry = narrow(jnp.int32(step), carry)
    psi_rows, both, carry = lax.optimization_barrier((psi_rows, both, carry))
    rotated = pl.pallas_call(
        functools.partial(rotate_body, row_tiles=row_tiles, tile_size=tile_size),
        out_shape=jax.ShapeDtypeStruct((g_rows * col_count, width), psi.dtype),
        grid=(1,),
        in_specs=[
            pl.BlockSpec((g_rows * col_count, bands), lambda i: (0, 0)),
            pl.BlockSpec((row_count, 1, g_rows, bands), lambda i: (0, 2, 0, 0)),
        ],
        out_specs=pl.BlockSpec((g_rows * col_count, width), lambda i: (0, 0)),
        compiler_params=pltpu.CompilerParams(vmem_limit_bytes=60 * MIB),
        name="rotate",
    )(psi_rows, both)
    recv, vecs, images, marks = narrow(jnp.int32(PB - 1), carry)

    updated = pl.pallas_call(
        functools.partial(last_body, row_count=row_count, col_count=col_count),
        out_shape=jax.ShapeDtypeStruct((height, width), F32),
        in_specs=[pl.BlockSpec(memory_space=pltpu.SMEM)]
        + [vmem() for _ in range(5)],
        out_specs=vmem(),
        scratch_shapes=[pltpu.VMEM(state.shape, F32), pltpu.VMEM(state.shape, F32)],
        compiler_params=pltpu.CompilerParams(vmem_limit_bytes=24 * MIB),
        name="update",
    )(where, recv, vecs, images, marks, tile)

    tile_shape = (row_tiles, 1, tile_size, col_tiles, 1, tile_size)
    return (
        correlation.reshape(tile_shape),
        updated.reshape(tile_shape),
        marks[0, :PB],
        marks[1, :PB],
        rotated.reshape(g_rows * col_count, col_tiles, 1, tile_size),
    )


def solution(mesh):
    return jax.shard_map(
        on_device,
        mesh=mesh,
        in_specs=(
            P(("row", "col"), None),
            P(("row", "col"), None),
            P(None, "row", None, None, "col", None),
        ),
        out_specs=(
            P(None, "row", None, None, "col", None),
            P(None, "row", None, None, "col", None),
            P(),
            P(),
            P("row", None, "col", None),
        ),
        check_vma=False,
    )
```

```python
import functools

import jax
import jax.numpy as jnp
from jax import lax
from jax.experimental import pallas as pl
from jax.experimental.pallas import tpu as pltpu
from jax.sharding import PartitionSpec as P

PB = 16
WIDE = 3
LANES = 128
F32 = jnp.float32
MIB = 1024 * 1024


def total(x):
    return jnp.sum(jnp.sum(x, axis=-2, keepdims=True), axis=-1, keepdims=True)


def over_k(left, right):
    return lax.dot_general(left, right, (((1,), (0,)), ((), ())), preferred_element_type=F32)


def products_body(where_ref, *refs, row_tiles, col_tiles, gvecs):
    rows = refs[:row_tiles]
    head_ref = refs[row_tiles]
    cols = refs[row_tiles + 1 : row_tiles + 1 + col_tiles]
    matrix_out, overlap_out, strip_out, left_vmem, left_psi_vmem = refs[row_tiles + 1 + col_tiles :]
    height = row_tiles * LANES

    def swapped(x):
        return jnp.concatenate([x[:, 1:2], x[:, 0:1]], axis=1).reshape(-1, LANES)

    @pl.when(pl.program_id(0) == 0)
    def _():
        for k, ref in enumerate(rows):
            at = pl.ds(k * LANES, LANES)
            left_vmem[at, :] = swapped(ref[...]).T
            left_psi_vmem[at, :] = ref[:, 0].reshape(-1, LANES).T
        left_vmem[height:, :] = swapped(head_ref[...]).T[:PB]

    both = jnp.concatenate([ref[...].reshape(-1, LANES) for ref in cols], axis=1)
    psi = jnp.concatenate([ref[:, 0].reshape(-1, LANES) for ref in cols], axis=1)
    mixed = 0.5 * over_k(left_vmem[...], both)
    matrix_out[0] = mixed[:height]
    strip_out[0] = mixed[height:]
    overlap_out[0] = over_k(left_psi_vmem[...], psi) * (1.0 / gvecs)


def gathered(recv_ref, row_count):
    recv = recv_ref[...]
    count = recv.shape[0] // row_count
    if count > 1:
        recv = jnp.sum(recv.reshape(row_count, count, *recv.shape[1:]), axis=1)
    return recv.reshape(1, -1, LANES)


def finish_image(image, vecs, images, vector, tau):
    along_w = total(images * vector)
    along_v = total(vecs * vector)
    image = image - jnp.sum(vecs * along_w + images * along_v, axis=0, keepdims=True)
    image = tau * image
    return image - 0.5 * tau * total(image * vector) * vector


def place(into, what, slot):
    slots = lax.broadcasted_iota(jnp.int32, (PB, 1, 1), 0)
    return jnp.where(slots == slot, what, into)


def spot_of(tile, row_count, row_tiles):
    return (tile % row_count) * row_tiles + tile // row_count


def step_body(
    step_ref, recv_ref, panel_ref, vecs_ref, images_ref, marks_ref, matrix_ref,
    vecs_out, images_out, marks_out, send_out, *, row_count,
):
    step = step_ref[0]
    tiles = vecs_ref.shape[1]
    col_count, height, width = matrix_ref.shape
    row_tiles = height // LANES
    col_tiles = width // LANES
    lane = lax.broadcasted_iota(jnp.int32, (1, 1, LANES), 2)
    marks = marks_ref[...]
    vecs = vecs_ref[...]
    images = images_ref[...]
    before = jnp.maximum(step - 1, 0)
    vector = vecs_ref[pl.ds(before, 1)]
    tau = marks[2:3, 0:1].reshape(1, 1, 1)
    image = finish_image(gathered(recv_ref, row_count), vecs, images, vector, tau)
    images = place(images, image, step - 1)
    images_out[...] = images
    head_w = jnp.sum(jnp.where(lane == step, images[:, 0:1, :], 0.0), axis=-1, keepdims=True)
    head_v = jnp.sum(jnp.where(lane == step, vecs[:, 0:1, :], 0.0), axis=-1, keepdims=True)
    column = panel_ref[pl.ds(step, 1)] - jnp.sum(
        vecs * head_w + images * head_v, axis=0, keepdims=True
    )
    shape = (1, tiles, LANES)
    spot = lax.broadcasted_iota(jnp.int32, shape, 1)
    tile = lax.div(spot, row_tiles) + lax.rem(spot, row_tiles) * row_count
    positions = tile * LANES + lax.broadcasted_iota(jnp.int32, shape, 2)
    below = positions > step + 1
    pivot = total(jnp.where(positions == step + 1, column, 0.0))
    tail = total(jnp.where(below, column * column, 0.0))
    corner = total(jnp.where(positions == step, column, 0.0))
    length = jnp.sqrt(pivot * pivot + tail)
    beta = jnp.where(pivot >= 0.0, -length, length)
    tau = (beta - pivot) / beta
    vector = jnp.where(positions == step + 1, 1.0, jnp.where(below, column / (pivot - beta), 0.0))
    vecs_out[...] = place(vecs, vector, step)
    row = lax.broadcasted_iota(jnp.int32, marks.shape, 0)
    mark = lax.broadcasted_iota(jnp.int32, marks.shape, 1) == step
    flat = marks.shape
    marks = jnp.where((row == 0) & mark, jnp.broadcast_to(corner[0], flat), marks)
    marks = jnp.where((row == 1) & mark, jnp.broadcast_to(beta[0], flat), marks)
    marks_out[...] = jnp.where(row == 2, jnp.broadcast_to(tau[0], flat), marks)
    sums = jnp.zeros((height, LANES), F32)
    for c in range(col_count):
        for a in range(col_tiles):
            at = spot_of(a * col_count + c, row_count, row_tiles)
            sums = sums + matrix_ref[c, :, a * LANES : (a + 1) * LANES] * vector[0, at : at + 1, :]
    send = jnp.concatenate(
        [
            jnp.sum(sums[k * LANES : (k + 1) * LANES].T, axis=0, keepdims=True)
            for k in range(row_tiles)
        ],
        axis=0,
    )
    send_out[...] = jnp.broadcast_to(send[None], send_out.shape)


def last_body(
    where_ref, recv_ref, vecs_ref, images_ref, marks_ref, tile_ref,
    updated_out, vecs_vmem, images_vmem, *, row_count, col_count,
):
    row_id = where_ref[0]
    col_id = where_ref[1]
    height, width = updated_out.shape
    row_tiles = height // LANES
    col_tiles = width // LANES
    vecs = vecs_ref[...]
    vector = vecs_ref[PB - 1 : PB]
    tau = marks_ref[2:3, 0:1].reshape(1, 1, 1)
    image = finish_image(gathered(recv_ref, row_count), vecs, images_ref[...], vector, tau)
    images_vmem[...] = place(images_ref[...], image, PB - 1)
    vecs_vmem[...] = vecs

    def part(ref, tile):
        at = lax.rem(tile, row_count) * row_tiles + lax.div(tile, row_count)
        return ref[:, pl.ds(at, 1), :].reshape(PB, LANES)

    lefts = [
        jnp.concatenate([part(vecs_vmem, at), part(images_vmem, at)], axis=0)
        for at in (row_id + k * row_count for k in range(row_tiles))
    ]
    rights = [
        jnp.concatenate([part(images_vmem, at), part(vecs_vmem, at)], axis=0)
        for at in (col_id + k * col_count for k in range(col_tiles))
    ]
    left = jnp.concatenate(lefts, axis=1)
    right = jnp.concatenate(rights, axis=1)
    change = lax.dot_general(
        left, right, (((0,), (0,)), ((), ())),
        precision=lax.Precision.HIGHEST, preferred_element_type=F32,
    )
    updated_out[...] = tile_ref[0] - change


def rotate_body(psi_ref, turn_ref, marks_ref, rotated_out):
    del marks_ref
    rotated_out[...] = over_k(psi_ref[...], turn_ref[...]).astype(rotated_out.dtype)


def vmem():
    return pl.BlockSpec(memory_space=pltpu.VMEM)


def on_device(psi, hpsi, eigvec):
    g_rows, bands = psi.shape
    row_tiles, _, tile_size, col_tiles = eigvec.shape[:4]
    row_count = lax.axis_size("row")
    col_count = lax.axis_size("col")
    devices = row_count * col_count
    row_id = lax.axis_index("row")
    col_id = lax.axis_index("col")
    gvecs = g_rows * devices
    height = row_tiles * tile_size
    width = col_tiles * tile_size
    tiles = bands // tile_size
    where = jnp.stack([row_id, col_id]).astype(jnp.int32)

    both = lax.all_gather(jnp.stack([psi, hpsi]), "row")
    turn = lax.all_gather(eigvec.reshape(row_tiles, tile_size, width), "row", axis=1)

    k = row_count * 2 * g_rows
    block = (row_count, 2, g_rows, tile_size)

    def column_block(index):
        return pl.BlockSpec(block, lambda c, where: (0, 0, 0, index(c, where)))

    in_specs = (
        [column_block(lambda c, where, a=a: where[0] + a * row_count) for a in range(row_tiles)]
        + [column_block(lambda c, where: 0)]
        + [column_block(lambda c, where, a=a: c + a * col_count) for a in range(col_tiles)]
    )
    blocks_shape = jax.ShapeDtypeStruct((col_count, height, width), F32)
    strip_shape = jax.ShapeDtypeStruct((col_count, PB, width), F32)
    matrix, overlap, strip = pl.pallas_call(
        functools.partial(products_body, row_tiles=row_tiles, col_tiles=col_tiles, gvecs=gvecs),
        out_shape=(blocks_shape, blocks_shape, strip_shape),
        grid_spec=pltpu.PrefetchScalarGridSpec(
            num_scalar_prefetch=1,
            grid=(col_count,),
            in_specs=in_specs,
            out_specs=tuple(
                pl.BlockSpec((1, *made.shape[1:]), lambda c, where: (c, 0, 0))
                for made in (blocks_shape, blocks_shape, strip_shape)
            ),
            scratch_shapes=[
                pltpu.VMEM((height + PB, k), psi.dtype),
                pltpu.VMEM((height, k // 2), psi.dtype),
            ],
        ),
        compiler_params=pltpu.CompilerParams(vmem_limit_bytes=60 * MIB),
        name="products",
    )(where, *([both] * len(in_specs)))

    turn, shared = lax.optimization_barrier((turn, matrix))
    summed = lax.psum(shared, "col")
    strip = lax.all_to_all(strip, "col", 0, 0, tiled=True)
    strip = jnp.sum(strip, axis=0)
    strip = lax.all_to_all(
        jnp.broadcast_to(strip[None], strip_shape.shape), "col", 0, 0, tiled=True
    )
    panel = jnp.transpose(
        strip.reshape(col_count, PB, row_tiles, col_tiles // row_tiles, tile_size), (1, 3, 0, 2, 4)
    ).reshape(PB, tiles, tile_size)

    state = jax.ShapeDtypeStruct((PB, tiles, tile_size), F32)
    marks_shape = jax.ShapeDtypeStruct((8, tile_size), F32)

    def advance(peers, step, recv, vecs, images, marks, factor):
        return pl.pallas_call(
            functools.partial(step_body, row_count=row_count),
            out_shape=(
                state, state, marks_shape,
                jax.ShapeDtypeStruct((peers, row_tiles, tile_size), F32),
            ),
            in_specs=[pl.BlockSpec(memory_space=pltpu.SMEM)]
            + [vmem() for _ in range(6)],
            out_specs=tuple(vmem() for _ in range(4)),
            input_output_aliases={3: 0, 4: 1, 5: 2},
            compiler_params=pltpu.CompilerParams(vmem_limit_bytes=24 * MIB),
            name="reflect",
        )(jnp.reshape(step, (1,)).astype(jnp.int32), recv, panel, vecs, images, marks, factor)

    def wide(step, carry):
        vecs, images, marks, send = advance(devices, step, *carry, matrix)
        return lax.all_to_all(send, ("row", "col"), 0, 0, tiled=True), vecs, images, marks

    def narrow(step, carry):
        vecs, images, marks, send = advance(row_count, step, *carry, summed)
        return lax.all_to_all(send, "row", 0, 0, tiled=True), vecs, images, marks

    carry = (
        jnp.zeros((devices, row_tiles, tile_size), F32),
        jnp.zeros(state.shape, F32),
        jnp.zeros(state.shape, F32),
        jnp.zeros(marks_shape.shape, F32),
    )
    carry = lax.fori_loop(0, WIDE, wide, carry)
    psi, overlap, carry = lax.optimization_barrier((psi, overlap, carry))
    psi_rows = lax.all_gather(psi, "col", axis=0, tiled=True)
    correlation = lax.psum_scatter(overlap, "col", scatter_dimension=0, tiled=True)
    for step in range(WIDE, PB - 1):
        carry = narrow(jnp.int32(step), carry)
    rotated = pl.pallas_call(
        rotate_body,
        out_shape=jax.ShapeDtypeStruct((g_rows * col_count, width), psi.dtype),
        grid=(1,),
        in_specs=[
            pl.BlockSpec((g_rows * col_count, bands), lambda i: (0, 0)),
            pl.BlockSpec((bands, width), lambda i: (0, 0)),
            pl.BlockSpec(marks_shape.shape, lambda i: (0, 0)),
        ],
        out_specs=pl.BlockSpec((g_rows * col_count, width), lambda i: (0, 0)),
        compiler_params=pltpu.CompilerParams(vmem_limit_bytes=24 * MIB),
        name="rotate",
    )(psi_rows, turn.reshape(bands, width), carry[3])
    recv, vecs, images, marks = narrow(jnp.int32(PB - 1), carry)

    def whole(shape):
        return pl.BlockSpec(shape, lambda i, where: (0,) * len(shape))

    updated = pl.pallas_call(
        functools.partial(last_body, row_count=row_count, col_count=col_count),
        out_shape=jax.ShapeDtypeStruct((height, width), F32),
        grid_spec=pltpu.PrefetchScalarGridSpec(
            num_scalar_prefetch=1,
            grid=(1,),
            in_specs=[
                whole(recv.shape),
                whole(state.shape),
                whole(state.shape),
                whole(marks_shape.shape),
                pl.BlockSpec((1, height, width), lambda i, where: (where[1], 0, 0)),
            ],
            out_specs=whole((height, width)),
            scratch_shapes=[pltpu.VMEM(state.shape, F32), pltpu.VMEM(state.shape, F32)],
        ),
        compiler_params=pltpu.CompilerParams(vmem_limit_bytes=24 * MIB),
        name="update",
    )(where, recv, vecs, images, marks, summed)

    tile_shape = (row_tiles, 1, tile_size, col_tiles, 1, tile_size)
    return (
        correlation.reshape(tile_shape),
        updated.reshape(tile_shape),
        marks[0, :PB],
        marks[1, :PB],
        rotated.reshape(g_rows * col_count, col_tiles, 1, tile_size),
    )


def solution(mesh):
    return jax.shard_map(
        on_device,
        mesh=mesh,
        in_specs=(
            P(("row", "col"), None),
            P(("row", "col"), None),
            P(None, "row", None, None, "col", None),
        ),
        out_specs=(
            P(None, "row", None, None, "col", None),
            P(None, "row", None, None, "col", None),
            P(),
            P(),
            P("row", None, "col", None),
        ),
        check_vma=False,
    )
```

```python
import functools

import jax
import jax.numpy as jnp
from jax import lax
from jax.experimental import pallas as pl
from jax.experimental.pallas import tpu as pltpu
from jax.sharding import PartitionSpec as P

PB = 16
WIDE = 2
LANES = 128
F32 = jnp.float32
MIB = 1024 * 1024


def total(x):
    return jnp.sum(jnp.sum(x, axis=-2, keepdims=True), axis=-1, keepdims=True)


def over_k(left, right):
    return lax.dot_general(left, right, (((1,), (0,)), ((), ())), preferred_element_type=F32)


def products_body(where_ref, *refs, row_tiles, col_tiles, gvecs):
    rows = refs[:row_tiles]
    head_ref = refs[row_tiles]
    cols = refs[row_tiles + 1 : row_tiles + 1 + col_tiles]
    matrix_out, overlap_out, strip_out, left_vmem, left_psi_vmem = refs[row_tiles + 1 + col_tiles :]
    height = row_tiles * LANES

    def swapped(x):
        return jnp.concatenate([x[:, 1:2], x[:, 0:1]], axis=1).reshape(-1, LANES)

    @pl.when(pl.program_id(0) == 0)
    def _():
        for k, ref in enumerate(rows):
            at = pl.ds(k * LANES, LANES)
            left_vmem[at, :] = swapped(ref[...]).T
            left_psi_vmem[at, :] = ref[:, 0].reshape(-1, LANES).T
        left_vmem[height:, :] = swapped(head_ref[...]).T[:PB]

    both = jnp.concatenate([ref[...].reshape(-1, LANES) for ref in cols], axis=1)
    psi = jnp.concatenate([ref[:, 0].reshape(-1, LANES) for ref in cols], axis=1)
    mixed = 0.5 * over_k(left_vmem[...], both)
    matrix_out[0] = mixed[:height]
    strip_out[0] = mixed[height:]
    overlap_out[0] = over_k(left_psi_vmem[...], psi) * (1.0 / gvecs)


def gathered(recv_ref, row_count):
    recv = recv_ref[...]
    count = recv.shape[0] // row_count
    if count > 1:
        recv = jnp.sum(recv.reshape(row_count, count, *recv.shape[1:]), axis=1)
    return recv.reshape(1, -1, LANES)


def finish_image(image, vecs, images, vector, tau):
    along_w = total(images * vector)
    along_v = total(vecs * vector)
    image = image - jnp.sum(vecs * along_w + images * along_v, axis=0, keepdims=True)
    image = tau * image
    return image - 0.5 * tau * total(image * vector) * vector


def place(into, what, slot):
    slots = lax.broadcasted_iota(jnp.int32, (PB, 1, 1), 0)
    return jnp.where(slots == slot, what, into)


def spot_of(tile, row_count, row_tiles):
    return (tile % row_count) * row_tiles + tile // row_count


def step_body(
    step_ref, recv_ref, panel_ref, vecs_ref, images_ref, marks_ref, matrix_ref,
    vecs_out, images_out, marks_out, send_out, *, row_count,
):
    step = step_ref[0]
    tiles = vecs_ref.shape[1]
    col_count, height, width = matrix_ref.shape
    row_tiles = height // LANES
    col_tiles = width // LANES
    lane = lax.broadcasted_iota(jnp.int32, (1, 1, LANES), 2)
    marks = marks_ref[...]
    vecs = vecs_ref[...]
    images = images_ref[...]
    before = jnp.maximum(step - 1, 0)
    vector = vecs_ref[pl.ds(before, 1)]
    tau = marks[2:3, 0:1].reshape(1, 1, 1)
    image = finish_image(gathered(recv_ref, row_count), vecs, images, vector, tau)
    images = place(images, image, step - 1)
    images_out[...] = images
    head_w = jnp.sum(jnp.where(lane == step, images[:, 0:1, :], 0.0), axis=-1, keepdims=True)
    head_v = jnp.sum(jnp.where(lane == step, vecs[:, 0:1, :], 0.0), axis=-1, keepdims=True)
    column = panel_ref[pl.ds(step, 1)] - jnp.sum(
        vecs * head_w + images * head_v, axis=0, keepdims=True
    )
    shape = (1, tiles, LANES)
    spot = lax.broadcasted_iota(jnp.int32, shape, 1)
    tile = lax.div(spot, row_tiles) + lax.rem(spot, row_tiles) * row_count
    positions = tile * LANES + lax.broadcasted_iota(jnp.int32, shape, 2)
    below = positions > step + 1
    pivot = total(jnp.where(positions == step + 1, column, 0.0))
    tail = total(jnp.where(below, column * column, 0.0))
    corner = total(jnp.where(positions == step, column, 0.0))
    length = jnp.sqrt(pivot * pivot + tail)
    beta = jnp.where(pivot >= 0.0, -length, length)
    tau = (beta - pivot) / beta
    vector = jnp.where(positions == step + 1, 1.0, jnp.where(below, column / (pivot - beta), 0.0))
    vecs_out[...] = place(vecs, vector, step)
    row = lax.broadcasted_iota(jnp.int32, marks.shape, 0)
    mark = lax.broadcasted_iota(jnp.int32, marks.shape, 1) == step
    flat = marks.shape
    marks = jnp.where((row == 0) & mark, jnp.broadcast_to(corner[0], flat), marks)
    marks = jnp.where((row == 1) & mark, jnp.broadcast_to(beta[0], flat), marks)
    marks_out[...] = jnp.where(row == 2, jnp.broadcast_to(tau[0], flat), marks)
    sums = jnp.zeros((height, LANES), F32)
    for c in range(col_count):
        for a in range(col_tiles):
            at = spot_of(a * col_count + c, row_count, row_tiles)
            sums = sums + matrix_ref[c, :, a * LANES : (a + 1) * LANES] * vector[0, at : at + 1, :]
    send = jnp.concatenate(
        [
            jnp.sum(sums[k * LANES : (k + 1) * LANES].T, axis=0, keepdims=True)
            for k in range(row_tiles)
        ],
        axis=0,
    )
    send_out[...] = jnp.broadcast_to(send[None], send_out.shape)


def last_body(
    where_ref, recv_ref, vecs_ref, images_ref, marks_ref, tile_ref,
    updated_out, vecs_vmem, images_vmem, *, row_count, col_count,
):
    row_id = where_ref[0]
    col_id = where_ref[1]
    height, width = updated_out.shape
    row_tiles = height // LANES
    col_tiles = width // LANES
    vecs = vecs_ref[...]
    vector = vecs_ref[PB - 1 : PB]
    tau = marks_ref[2:3, 0:1].reshape(1, 1, 1)
    image = finish_image(gathered(recv_ref, row_count), vecs, images_ref[...], vector, tau)
    images_vmem[...] = place(images_ref[...], image, PB - 1)
    vecs_vmem[...] = vecs

    def part(ref, tile):
        at = lax.rem(tile, row_count) * row_tiles + lax.div(tile, row_count)
        return ref[:, pl.ds(at, 1), :].reshape(PB, LANES)

    lefts = [
        jnp.concatenate([part(vecs_vmem, at), part(images_vmem, at)], axis=0)
        for at in (row_id + k * row_count for k in range(row_tiles))
    ]
    rights = [
        jnp.concatenate([part(images_vmem, at), part(vecs_vmem, at)], axis=0)
        for at in (col_id + k * col_count for k in range(col_tiles))
    ]
    left = jnp.concatenate(lefts, axis=1)
    right = jnp.concatenate(rights, axis=1)
    change = lax.dot_general(
        left, right, (((0,), (0,)), ((), ())),
        precision=lax.Precision.HIGHEST, preferred_element_type=F32,
    )
    updated_out[...] = tile_ref[0] - change


def rotate_body(psi_ref, both_ref, marks_ref, rotated_out, *, row_tiles, tile_size):
    del marks_ref
    row_count, _, g_rows, bands = both_ref.shape
    width = rotated_out.shape[1]
    pieces = tile_size // g_rows
    sums = jnp.zeros(rotated_out.shape, F32)
    for a in range(row_tiles):
        for r in range(0, row_count, 2):
            turn = jnp.concatenate(
                [
                    both_ref[q, 0, :, (a * pieces + s) * width : (a * pieces + s + 1) * width]
                    for q in (r, r + 1)
                    for s in range(pieces)
                ],
                axis=0,
            )
            at = (a * row_count + r) * tile_size
            sums = sums + over_k(psi_ref[:, at : at + 2 * tile_size], turn)
    rotated_out[...] = sums.astype(rotated_out.dtype)


def vmem():
    return pl.BlockSpec(memory_space=pltpu.VMEM)


def on_device(psi, hpsi, eigvec):
    g_rows, bands = psi.shape
    row_tiles, _, tile_size, col_tiles = eigvec.shape[:4]
    row_count = lax.axis_size("row")
    col_count = lax.axis_size("col")
    devices = row_count * col_count
    row_id = lax.axis_index("row")
    col_id = lax.axis_index("col")
    gvecs = g_rows * devices
    height = row_tiles * tile_size
    width = col_tiles * tile_size
    tiles = bands // tile_size
    where = jnp.stack([row_id, col_id]).astype(jnp.int32)

    lanes = bands // width
    folded = jnp.transpose(eigvec.reshape(lanes, g_rows, width), (1, 0, 2)).reshape(g_rows, bands)
    both = lax.all_gather(jnp.stack([psi, hpsi, folded]), "row")

    k = row_count * 2 * g_rows
    block = (row_count, 2, g_rows, tile_size)

    def column_block(index):
        return pl.BlockSpec(block, lambda c, where: (0, 0, 0, index(c, where)))

    in_specs = (
        [column_block(lambda c, where, a=a: where[0] + a * row_count) for a in range(row_tiles)]
        + [column_block(lambda c, where: 0)]
        + [column_block(lambda c, where, a=a: c + a * col_count) for a in range(col_tiles)]
    )
    blocks_shape = jax.ShapeDtypeStruct((col_count, height, width), F32)
    strip_shape = jax.ShapeDtypeStruct((col_count, PB, width), F32)
    matrix, overlap, strip = pl.pallas_call(
        functools.partial(products_body, row_tiles=row_tiles, col_tiles=col_tiles, gvecs=gvecs),
        out_shape=(blocks_shape, blocks_shape, strip_shape),
        grid_spec=pltpu.PrefetchScalarGridSpec(
            num_scalar_prefetch=1,
            grid=(col_count,),
            in_specs=in_specs,
            out_specs=tuple(
                pl.BlockSpec((1, *made.shape[1:]), lambda c, where: (c, 0, 0))
                for made in (blocks_shape, blocks_shape, strip_shape)
            ),
            scratch_shapes=[
                pltpu.VMEM((height + PB, k), psi.dtype),
                pltpu.VMEM((height, k // 2), psi.dtype),
            ],
        ),
        compiler_params=pltpu.CompilerParams(vmem_limit_bytes=60 * MIB),
        name="products",
    )(where, *([both] * len(in_specs)))

    summed = lax.psum(matrix, "col")
    strip = lax.all_to_all(strip, "col", 0, 0, tiled=True)
    strip = jnp.sum(strip, axis=0)
    strip = lax.all_to_all(
        jnp.broadcast_to(strip[None], strip_shape.shape), "col", 0, 0, tiled=True
    )
    panel = jnp.transpose(
        strip.reshape(col_count, PB, row_tiles, col_tiles // row_tiles, tile_size), (1, 3, 0, 2, 4)
    ).reshape(PB, tiles, tile_size)

    state = jax.ShapeDtypeStruct((PB, tiles, tile_size), F32)
    marks_shape = jax.ShapeDtypeStruct((8, tile_size), F32)

    def advance(peers, step, recv, vecs, images, marks, factor):
        return pl.pallas_call(
            functools.partial(step_body, row_count=row_count),
            out_shape=(
                state, state, marks_shape,
                jax.ShapeDtypeStruct((peers, row_tiles, tile_size), F32),
            ),
            in_specs=[pl.BlockSpec(memory_space=pltpu.SMEM)]
            + [vmem() for _ in range(6)],
            out_specs=tuple(vmem() for _ in range(4)),
            input_output_aliases={3: 0, 4: 1, 5: 2},
            compiler_params=pltpu.CompilerParams(vmem_limit_bytes=24 * MIB),
            name="reflect",
        )(jnp.reshape(step, (1,)).astype(jnp.int32), recv, panel, vecs, images, marks, factor)

    def wide(step, carry):
        vecs, images, marks, send = advance(devices, step, *carry, matrix)
        return lax.all_to_all(send, ("row", "col"), 0, 0, tiled=True), vecs, images, marks

    def narrow(step, carry):
        vecs, images, marks, send = advance(row_count, step, *carry, summed)
        return lax.all_to_all(send, "row", 0, 0, tiled=True), vecs, images, marks

    carry = (
        jnp.zeros((devices, row_tiles, tile_size), F32),
        jnp.zeros(state.shape, F32),
        jnp.zeros(state.shape, F32),
        jnp.zeros(marks_shape.shape, F32),
    )
    carry = lax.fori_loop(0, WIDE, wide, carry)
    psi, overlap, carry = lax.optimization_barrier((psi, overlap, carry))
    psi_rows = lax.all_gather(psi, "col", axis=0, tiled=True)
    correlation = lax.psum_scatter(overlap, "col", scatter_dimension=0, tiled=True)
    for step in range(WIDE, PB - 1):
        carry = narrow(jnp.int32(step), carry)
    rotated = pl.pallas_call(
        functools.partial(rotate_body, row_tiles=row_tiles, tile_size=tile_size),
        out_shape=jax.ShapeDtypeStruct((g_rows * col_count, width), psi.dtype),
        grid=(1,),
        in_specs=[
            pl.BlockSpec((g_rows * col_count, bands), lambda i: (0, 0)),
            pl.BlockSpec((row_count, 1, g_rows, bands), lambda i: (0, 2, 0, 0)),
            pl.BlockSpec(marks_shape.shape, lambda i: (0, 0)),
        ],
        out_specs=pl.BlockSpec((g_rows * col_count, width), lambda i: (0, 0)),
        compiler_params=pltpu.CompilerParams(vmem_limit_bytes=60 * MIB),
        name="rotate",
    )(psi_rows, both, carry[3])
    recv, vecs, images, marks = narrow(jnp.int32(PB - 1), carry)

    def whole(shape):
        return pl.BlockSpec(shape, lambda i, where: (0,) * len(shape))

    updated = pl.pallas_call(
        functools.partial(last_body, row_count=row_count, col_count=col_count),
        out_shape=jax.ShapeDtypeStruct((height, width), F32),
        grid_spec=pltpu.PrefetchScalarGridSpec(
            num_scalar_prefetch=1,
            grid=(1,),
            in_specs=[
                whole(recv.shape),
                whole(state.shape),
                whole(state.shape),
                whole(marks_shape.shape),
                pl.BlockSpec((1, height, width), lambda i, where: (where[1], 0, 0)),
            ],
            out_specs=whole((height, width)),
            scratch_shapes=[pltpu.VMEM(state.shape, F32), pltpu.VMEM(state.shape, F32)],
        ),
        compiler_params=pltpu.CompilerParams(vmem_limit_bytes=60 * MIB),
        name="update",
    )(where, recv, vecs, images, marks, summed)

    tile_shape = (row_tiles, 1, tile_size, col_tiles, 1, tile_size)
    return (
        correlation.reshape(tile_shape),
        updated.reshape(tile_shape),
        marks[0, :PB],
        marks[1, :PB],
        rotated.reshape(g_rows * col_count, col_tiles, 1, tile_size),
    )


def solution(mesh):
    return jax.shard_map(
        on_device,
        mesh=mesh,
        in_specs=(
            P(("row", "col"), None),
            P(("row", "col"), None),
            P(None, "row", None, None, "col", None),
        ),
        out_specs=(
            P(None, "row", None, None, "col", None),
            P(None, "row", None, None, "col", None),
            P(),
            P(),
            P("row", None, "col", None),
        ),
        check_vma=False,
    )
```

```python
import functools

import jax
import jax.numpy as jnp
from jax import lax
from jax.experimental import pallas as pl
from jax.experimental.pallas import tpu as pltpu
from jax.sharding import PartitionSpec as P

PB = 16
WIDE = 2
LANES = 128
F32 = jnp.float32
MIB = 1024 * 1024


def total(x):
    return jnp.sum(jnp.sum(x, axis=-2, keepdims=True), axis=-1, keepdims=True)


def over_k(left, right):
    return lax.dot_general(left, right, (((1,), (0,)), ((), ())), preferred_element_type=F32)


def matrix_body(where_ref, *refs, row_tiles, col_tiles):
    rows = refs[:row_tiles]
    head_ref = refs[row_tiles]
    cols = refs[row_tiles + 1 : row_tiles + 1 + col_tiles]
    matrix_out, strip_out, left_vmem = refs[row_tiles + 1 + col_tiles :]
    height = row_tiles * LANES

    def swapped(x):
        return jnp.concatenate([x[:, 1:2], x[:, 0:1]], axis=1).reshape(-1, LANES)

    @pl.when(pl.program_id(0) == 0)
    def _():
        for k, ref in enumerate(rows):
            left_vmem[pl.ds(k * LANES, LANES), :] = swapped(ref[...]).T
        left_vmem[height:, :] = swapped(head_ref[...]).T[:PB]

    both = jnp.concatenate([ref[...].reshape(-1, LANES) for ref in cols], axis=1)
    mixed = 0.5 * over_k(left_vmem[...], both)
    matrix_out[0] = mixed[:height]
    strip_out[0] = mixed[height:]


def overlap_body(where_ref, *refs, row_tiles, col_tiles, gvecs):
    rows = refs[:row_tiles]
    cols = refs[row_tiles : row_tiles + col_tiles]
    overlap_out, left_vmem = refs[row_tiles + col_tiles :]

    @pl.when(pl.program_id(0) == 0)
    def _():
        for k, ref in enumerate(rows):
            left_vmem[pl.ds(k * LANES, LANES), :] = ref[...].reshape(-1, LANES).T

    psi = jnp.concatenate([ref[...].reshape(-1, LANES) for ref in cols], axis=1)
    overlap_out[0] = over_k(left_vmem[...], psi) * (1.0 / gvecs)


def gathered(recv_ref, row_count):
    recv = recv_ref[...]
    count = recv.shape[0] // row_count
    if count > 1:
        recv = jnp.sum(recv.reshape(row_count, count, *recv.shape[1:]), axis=1)
    return recv.reshape(1, -1, LANES)


def finish_image(image, vecs, images, vector, tau):
    along_w = total(images * vector)
    along_v = total(vecs * vector)
    image = image - jnp.sum(vecs * along_w + images * along_v, axis=0, keepdims=True)
    image = tau * image
    return image - 0.5 * tau * total(image * vector) * vector


def place(into, what, slot):
    slots = lax.broadcasted_iota(jnp.int32, (PB, 1, 1), 0)
    return jnp.where(slots == slot, what, into)


def spot_of(tile, row_count, row_tiles):
    return (tile % row_count) * row_tiles + tile // row_count


def step_body(
    step_ref, recv_ref, panel_ref, vecs_ref, images_ref, marks_ref, matrix_ref,
    vecs_out, images_out, marks_out, send_out, *, row_count,
):
    step = step_ref[0]
    tiles = vecs_ref.shape[1]
    col_count, height, width = matrix_ref.shape
    row_tiles = height // LANES
    col_tiles = width // LANES
    lane = lax.broadcasted_iota(jnp.int32, (1, 1, LANES), 2)
    marks = marks_ref[...]
    vecs = vecs_ref[...]
    images = images_ref[...]
    before = jnp.maximum(step - 1, 0)
    vector = vecs_ref[pl.ds(before, 1)]
    tau = marks[2:3, 0:1].reshape(1, 1, 1)
    image = finish_image(gathered(recv_ref, row_count), vecs, images, vector, tau)
    images = place(images, image, step - 1)
    images_out[...] = images
    head_w = jnp.sum(jnp.where(lane == step, images[:, 0:1, :], 0.0), axis=-1, keepdims=True)
    head_v = jnp.sum(jnp.where(lane == step, vecs[:, 0:1, :], 0.0), axis=-1, keepdims=True)
    column = panel_ref[pl.ds(step, 1)] - jnp.sum(
        vecs * head_w + images * head_v, axis=0, keepdims=True
    )
    shape = (1, tiles, LANES)
    spot = lax.broadcasted_iota(jnp.int32, shape, 1)
    tile = lax.div(spot, row_tiles) + lax.rem(spot, row_tiles) * row_count
    positions = tile * LANES + lax.broadcasted_iota(jnp.int32, shape, 2)
    below = positions > step + 1
    pivot = total(jnp.where(positions == step + 1, column, 0.0))
    tail = total(jnp.where(below, column * column, 0.0))
    corner = total(jnp.where(positions == step, column, 0.0))
    length = jnp.sqrt(pivot * pivot + tail)
    beta = jnp.where(pivot >= 0.0, -length, length)
    tau = (beta - pivot) / beta
    vector = jnp.where(positions == step + 1, 1.0, jnp.where(below, column / (pivot - beta), 0.0))
    vecs_out[...] = place(vecs, vector, step)
    row = lax.broadcasted_iota(jnp.int32, marks.shape, 0)
    mark = lax.broadcasted_iota(jnp.int32, marks.shape, 1) == step
    flat = marks.shape
    marks = jnp.where((row == 0) & mark, jnp.broadcast_to(corner[0], flat), marks)
    marks = jnp.where((row == 1) & mark, jnp.broadcast_to(beta[0], flat), marks)
    marks_out[...] = jnp.where(row == 2, jnp.broadcast_to(tau[0], flat), marks)
    sums = jnp.zeros((height, LANES), F32)
    for c in range(col_count):
        for a in range(col_tiles):
            at = spot_of(a * col_count + c, row_count, row_tiles)
            sums = sums + matrix_ref[c, :, a * LANES : (a + 1) * LANES] * vector[0, at : at + 1, :]
    send = jnp.concatenate(
        [
            jnp.sum(sums[k * LANES : (k + 1) * LANES].T, axis=0, keepdims=True)
            for k in range(row_tiles)
        ],
        axis=0,
    )
    send_out[...] = jnp.broadcast_to(send[None], send_out.shape)


def last_body(
    where_ref, recv_ref, vecs_ref, images_ref, marks_ref, tile_ref,
    updated_out, vecs_vmem, images_vmem, *, row_count, col_count,
):
    row_id = where_ref[0]
    col_id = where_ref[1]
    height, width = updated_out.shape
    row_tiles = height // LANES
    col_tiles = width // LANES
    vecs = vecs_ref[...]
    vector = vecs_ref[PB - 1 : PB]
    tau = marks_ref[2:3, 0:1].reshape(1, 1, 1)
    image = finish_image(gathered(recv_ref, row_count), vecs, images_ref[...], vector, tau)
    images_vmem[...] = place(images_ref[...], image, PB - 1)
    vecs_vmem[...] = vecs

    def part(ref, tile):
        at = lax.rem(tile, row_count) * row_tiles + lax.div(tile, row_count)
        return ref[:, pl.ds(at, 1), :].reshape(PB, LANES)

    lefts = [
        jnp.concatenate([part(vecs_vmem, at), part(images_vmem, at)], axis=0)
        for at in (row_id + k * row_count for k in range(row_tiles))
    ]
    rights = [
        jnp.concatenate([part(images_vmem, at), part(vecs_vmem, at)], axis=0)
        for at in (col_id + k * col_count for k in range(col_tiles))
    ]
    left = jnp.concatenate(lefts, axis=1)
    right = jnp.concatenate(rights, axis=1)
    change = lax.dot_general(
        left, right, (((0,), (0,)), ((), ())),
        precision=lax.Precision.HIGHEST, preferred_element_type=F32,
    )
    updated_out[...] = tile_ref[...] - change


def rotate_body(
    where_ref, psi_ref, both_ref, marks_ref, block_ref, rotated_out, tile_out, *, row_tiles, tile_size
):
    del where_ref, marks_ref
    tile_out[...] = block_ref[0]
    row_count, _, g_rows, bands = both_ref.shape
    width = rotated_out.shape[1]
    pieces = tile_size // g_rows
    sums = jnp.zeros(rotated_out.shape, F32)
    for a in range(row_tiles):
        for r in range(0, row_count, 2):
            turn = jnp.concatenate(
                [
                    both_ref[q, 0, :, (a * pieces + s) * width : (a * pieces + s + 1) * width]
                    for q in (r, r + 1)
                    for s in range(pieces)
                ],
                axis=0,
            )
            at = (a * row_count + r) * tile_size
            sums = sums + over_k(psi_ref[:, at : at + 2 * tile_size], turn)
    rotated_out[...] = sums.astype(rotated_out.dtype)


def vmem():
    return pl.BlockSpec(memory_space=pltpu.VMEM)


def on_device(psi, hpsi, eigvec):
    g_rows, bands = psi.shape
    row_tiles, _, tile_size, col_tiles = eigvec.shape[:4]
    row_count = lax.axis_size("row")
    col_count = lax.axis_size("col")
    devices = row_count * col_count
    row_id = lax.axis_index("row")
    col_id = lax.axis_index("col")
    gvecs = g_rows * devices
    height = row_tiles * tile_size
    width = col_tiles * tile_size
    tiles = bands // tile_size
    where = jnp.stack([row_id, col_id]).astype(jnp.int32)

    lanes = bands // width
    folded = jnp.transpose(eigvec.reshape(lanes, g_rows, width), (1, 0, 2)).reshape(g_rows, bands)
    both = lax.all_gather(jnp.stack([psi, hpsi, folded]), "row")

    blocks_shape = jax.ShapeDtypeStruct((col_count, height, width), F32)
    strip_shape = jax.ShapeDtypeStruct((col_count, PB, width), F32)

    def products(body, source, kinds, with_head, made, name):
        def column_block(index):
            return pl.BlockSpec(
                (row_count, kinds, g_rows, tile_size), lambda c, where: (0, 0, 0, index(c, where))
            )

        in_specs = [
            column_block(lambda c, where, a=a: where[0] + a * row_count) for a in range(row_tiles)
        ]
        if with_head:
            in_specs.append(column_block(lambda c, where: 0))
        in_specs += [
            column_block(lambda c, where, a=a: c + a * col_count) for a in range(col_tiles)
        ]
        left = (height + PB * with_head, row_count * kinds * g_rows)
        return pl.pallas_call(
            body,
            out_shape=made,
            grid_spec=pltpu.PrefetchScalarGridSpec(
                num_scalar_prefetch=1,
                grid=(col_count,),
                in_specs=in_specs,
                out_specs=tuple(
                    pl.BlockSpec((1, *one.shape[1:]), lambda c, where: (c, 0, 0)) for one in made
                ),
                scratch_shapes=[pltpu.VMEM(left, psi.dtype)],
            ),
            compiler_params=pltpu.CompilerParams(vmem_limit_bytes=60 * MIB),
            name=name,
        )(where, *([source] * len(in_specs)))

    matrix, strip = products(
        functools.partial(matrix_body, row_tiles=row_tiles, col_tiles=col_tiles),
        both, 2, 1, (blocks_shape, strip_shape), "products",
    )

    summed = lax.psum(matrix, "col")
    strip = lax.all_to_all(strip, "col", 0, 0, tiled=True)
    strip = jnp.sum(strip, axis=0)
    strip = lax.all_to_all(
        jnp.broadcast_to(strip[None], strip_shape.shape), "col", 0, 0, tiled=True
    )
    (overlap,) = products(
        functools.partial(
            overlap_body, row_tiles=row_tiles, col_tiles=col_tiles, gvecs=gvecs
        ),
        both, 1, 0, (blocks_shape,), "overlaps",
    )
    panel = jnp.transpose(
        strip.reshape(col_count, PB, row_tiles, col_tiles // row_tiles, tile_size), (1, 3, 0, 2, 4)
    ).reshape(PB, tiles, tile_size)

    state = jax.ShapeDtypeStruct((PB, tiles, tile_size), F32)
    marks_shape = jax.ShapeDtypeStruct((8, tile_size), F32)

    def advance(peers, step, recv, vecs, images, marks, factor):
        return pl.pallas_call(
            functools.partial(step_body, row_count=row_count),
            out_shape=(
                state, state, marks_shape,
                jax.ShapeDtypeStruct((peers, row_tiles, tile_size), F32),
            ),
            in_specs=[pl.BlockSpec(memory_space=pltpu.SMEM)]
            + [vmem() for _ in range(6)],
            out_specs=tuple(vmem() for _ in range(4)),
            input_output_aliases={3: 0, 4: 1, 5: 2},
            compiler_params=pltpu.CompilerParams(vmem_limit_bytes=24 * MIB),
            name="reflect",
        )(jnp.reshape(step, (1,)).astype(jnp.int32), recv, panel, vecs, images, marks, factor)

    def wide(step, carry):
        vecs, images, marks, send = advance(devices, step, *carry, matrix)
        return lax.all_to_all(send, ("row", "col"), 0, 0, tiled=True), vecs, images, marks

    def narrow(step, carry):
        vecs, images, marks, send = advance(row_count, step, *carry, summed)
        return lax.all_to_all(send, "row", 0, 0, tiled=True), vecs, images, marks

    carry = (
        jnp.zeros((devices, row_tiles, tile_size), F32),
        jnp.zeros(state.shape, F32),
        jnp.zeros(state.shape, F32),
        jnp.zeros(marks_shape.shape, F32),
    )
    carry = lax.fori_loop(0, WIDE, wide, carry)
    psi, overlap, carry = lax.optimization_barrier((psi, overlap, carry))
    psi_rows = lax.all_gather(psi, "col", axis=0, tiled=True)
    correlation = lax.psum_scatter(overlap, "col", scatter_dimension=0, tiled=True)
    for step in range(WIDE, PB - 1):
        carry = narrow(jnp.int32(step), carry)
    rotated, tile = pl.pallas_call(
        functools.partial(rotate_body, row_tiles=row_tiles, tile_size=tile_size),
        out_shape=(
            jax.ShapeDtypeStruct((g_rows * col_count, width), psi.dtype),
            jax.ShapeDtypeStruct((height, width), F32),
        ),
        grid_spec=pltpu.PrefetchScalarGridSpec(
            num_scalar_prefetch=1,
            grid=(1,),
            in_specs=[
                pl.BlockSpec((g_rows * col_count, bands), lambda i, where: (0, 0)),
                pl.BlockSpec((row_count, 1, g_rows, bands), lambda i, where: (0, 2, 0, 0)),
                pl.BlockSpec(marks_shape.shape, lambda i, where: (0, 0)),
                pl.BlockSpec((1, height, width), lambda i, where: (where[1], 0, 0)),
            ],
            out_specs=(
                pl.BlockSpec((g_rows * col_count, width), lambda i, where: (0, 0)),
                pl.BlockSpec((height, width), lambda i, where: (0, 0)),
            ),
        ),
        compiler_params=pltpu.CompilerParams(vmem_limit_bytes=60 * MIB),
        name="rotate",
    )(where, psi_rows, both, carry[3], summed)
    recv, vecs, images, marks = narrow(jnp.int32(PB - 1), carry)

    updated = pl.pallas_call(
        functools.partial(last_body, row_count=row_count, col_count=col_count),
        out_shape=jax.ShapeDtypeStruct((height, width), F32),
        in_specs=[pl.BlockSpec(memory_space=pltpu.SMEM)] + [vmem() for _ in range(5)],
        out_specs=vmem(),
        scratch_shapes=[pltpu.VMEM(state.shape, F32), pltpu.VMEM(state.shape, F32)],
        compiler_params=pltpu.CompilerParams(vmem_limit_bytes=24 * MIB),
        name="update",
    )(where, recv, vecs, images, marks, tile)

    tile_shape = (row_tiles, 1, tile_size, col_tiles, 1, tile_size)
    return (
        correlation.reshape(tile_shape),
        updated.reshape(tile_shape),
        marks[0, :PB],
        marks[1, :PB],
        rotated.reshape(g_rows * col_count, col_tiles, 1, tile_size),
    )


def solution(mesh):
    return jax.shard_map(
        on_device,
        mesh=mesh,
        in_specs=(
            P(("row", "col"), None),
            P(("row", "col"), None),
            P(None, "row", None, None, "col", None),
        ),
        out_specs=(
            P(None, "row", None, None, "col", None),
            P(None, "row", None, None, "col", None),
            P(),
            P(),
            P("row", None, "col", None),
        ),
        check_vma=False,
    )
```

```python
import functools

import jax
import jax.numpy as jnp
from jax import lax
from jax.experimental import pallas as pl
from jax.experimental.pallas import tpu as pltpu
from jax.sharding import PartitionSpec as P

PB = 16
WIDE = 2
LANES = 128
F32 = jnp.float32
MIB = 1024 * 1024


def total(x):
    return jnp.sum(jnp.sum(x, axis=-2, keepdims=True), axis=-1, keepdims=True)


def over_k(left, right):
    return lax.dot_general(left, right, (((1,), (0,)), ((), ())), preferred_element_type=F32)


def matrix_body(where_ref, *refs, row_tiles):
    rows = refs[:row_tiles]
    head_ref, cols_ref, matrix_out, strip_out, left_vmem = refs[row_tiles:]
    height = row_tiles * LANES

    def swapped(x):
        return jnp.concatenate([x[:, 1:2], x[:, 0:1]], axis=1).reshape(-1, LANES)

    @pl.when(pl.program_id(0) == 0)
    def _():
        for k, ref in enumerate(rows):
            left_vmem[pl.ds(k * LANES, LANES), :] = swapped(ref[...]).T
        left_vmem[height:, :] = swapped(head_ref[...]).T[:PB]

    both = cols_ref[...].reshape(left_vmem.shape[1], -1)
    mixed = 0.5 * over_k(left_vmem[...], both)
    matrix_out[0] = mixed[:height]
    strip_out[0] = mixed[height:]


def overlap_body(where_ref, *refs, row_tiles, col_tiles, gvecs):
    rows = refs[:row_tiles]
    cols = refs[row_tiles : row_tiles + col_tiles]
    overlap_out, left_vmem = refs[row_tiles + col_tiles :]

    @pl.when(pl.program_id(0) == 0)
    def _():
        for k, ref in enumerate(rows):
            left_vmem[pl.ds(k * LANES, LANES), :] = ref[...].reshape(-1, LANES).T

    psi = jnp.concatenate([ref[...].reshape(-1, LANES) for ref in cols], axis=1)
    overlap_out[0] = over_k(left_vmem[...], psi) * (1.0 / gvecs)


def gathered(recv_ref, row_count):
    recv = recv_ref[...]
    count = recv.shape[0] // row_count
    if count > 1:
        recv = jnp.sum(recv.reshape(row_count, count, *recv.shape[1:]), axis=1)
    return recv.reshape(1, -1, LANES)


def finish_image(image, vecs, images, vector, tau):
    along_w = total(images * vector)
    along_v = total(vecs * vector)
    image = image - jnp.sum(vecs * along_w + images * along_v, axis=0, keepdims=True)
    image = tau * image
    return image - 0.5 * tau * total(image * vector) * vector


def place(into, what, slot):
    slots = lax.broadcasted_iota(jnp.int32, (PB, 1, 1), 0)
    return jnp.where(slots == slot, what, into)


def spot_of(tile, row_count, row_tiles):
    return (tile % row_count) * row_tiles + tile // row_count


def step_body(
    step_ref, recv_ref, panel_ref, vecs_ref, images_ref, marks_ref, matrix_ref,
    vecs_out, images_out, marks_out, send_out, *, row_count,
):
    step = step_ref[0]
    tiles = vecs_ref.shape[1]
    col_count, height, width = matrix_ref.shape
    row_tiles = height // LANES
    col_tiles = width // LANES
    lane = lax.broadcasted_iota(jnp.int32, (1, 1, LANES), 2)
    marks = marks_ref[...]
    vecs = vecs_ref[...]
    images = images_ref[...]
    before = jnp.maximum(step - 1, 0)
    vector = vecs_ref[pl.ds(before, 1)]
    tau = marks[2:3, 0:1].reshape(1, 1, 1)
    image = finish_image(gathered(recv_ref, row_count), vecs, images, vector, tau)
    images = place(images, image, step - 1)
    images_out[...] = images
    head_w = jnp.sum(jnp.where(lane == step, images[:, 0:1, :], 0.0), axis=-1, keepdims=True)
    head_v = jnp.sum(jnp.where(lane == step, vecs[:, 0:1, :], 0.0), axis=-1, keepdims=True)
    column = panel_ref[pl.ds(step, 1)] - jnp.sum(
        vecs * head_w + images * head_v, axis=0, keepdims=True
    )
    shape = (1, tiles, LANES)
    spot = lax.broadcasted_iota(jnp.int32, shape, 1)
    tile = lax.div(spot, row_tiles) + lax.rem(spot, row_tiles) * row_count
    positions = tile * LANES + lax.broadcasted_iota(jnp.int32, shape, 2)
    below = positions > step + 1
    pivot = total(jnp.where(positions == step + 1, column, 0.0))
    tail = total(jnp.where(below, column * column, 0.0))
    corner = total(jnp.where(positions == step, column, 0.0))
    length = jnp.sqrt(pivot * pivot + tail)
    beta = jnp.where(pivot >= 0.0, -length, length)
    tau = (beta - pivot) / beta
    vector = jnp.where(positions == step + 1, 1.0, jnp.where(below, column / (pivot - beta), 0.0))
    vecs_out[...] = place(vecs, vector, step)
    row = lax.broadcasted_iota(jnp.int32, marks.shape, 0)
    mark = lax.broadcasted_iota(jnp.int32, marks.shape, 1) == step
    flat = marks.shape
    marks = jnp.where((row == 0) & mark, jnp.broadcast_to(corner[0], flat), marks)
    marks = jnp.where((row == 1) & mark, jnp.broadcast_to(beta[0], flat), marks)
    marks_out[...] = jnp.where(row == 2, jnp.broadcast_to(tau[0], flat), marks)
    sums = jnp.zeros((height, LANES), F32)
    for c in range(col_count):
        for a in range(col_tiles):
            at = spot_of(c * col_tiles + a, row_count, row_tiles)
            sums = sums + matrix_ref[c, :, a * LANES : (a + 1) * LANES] * vector[0, at : at + 1, :]
    send = jnp.concatenate(
        [
            jnp.sum(sums[k * LANES : (k + 1) * LANES].T, axis=0, keepdims=True)
            for k in range(row_tiles)
        ],
        axis=0,
    )
    send_out[...] = jnp.broadcast_to(send[None], send_out.shape)


def last_body(
    where_ref, recv_ref, vecs_ref, images_ref, marks_ref, tile_ref,
    updated_out, vecs_vmem, images_vmem, *, row_count, col_count,
):
    row_id = where_ref[0]
    col_id = where_ref[1]
    height, width = updated_out.shape
    row_tiles = height // LANES
    col_tiles = width // LANES
    vecs = vecs_ref[...]
    vector = vecs_ref[PB - 1 : PB]
    tau = marks_ref[2:3, 0:1].reshape(1, 1, 1)
    image = finish_image(gathered(recv_ref, row_count), vecs, images_ref[...], vector, tau)
    images_vmem[...] = place(images_ref[...], image, PB - 1)
    vecs_vmem[...] = vecs

    def part(ref, tile):
        at = lax.rem(tile, row_count) * row_tiles + lax.div(tile, row_count)
        return ref[:, pl.ds(at, 1), :].reshape(PB, LANES)

    lefts = [
        jnp.concatenate([part(vecs_vmem, at), part(images_vmem, at)], axis=0)
        for at in (row_id + k * row_count for k in range(row_tiles))
    ]
    rights = [
        jnp.concatenate([part(images_vmem, at), part(vecs_vmem, at)], axis=0)
        for at in (col_id + k * col_count for k in range(col_tiles))
    ]
    left = jnp.concatenate(lefts, axis=1)
    right = jnp.concatenate(rights, axis=1)
    change = lax.dot_general(
        left, right, (((0,), (0,)), ((), ())),
        precision=lax.Precision.HIGHEST, preferred_element_type=F32,
    )
    updated_out[...] = tile_ref[...] - change


def rotate_body(
    where_ref, psi_ref, both_ref, marks_ref, *refs, row_tiles, tile_size
):
    *blocks, rotated_out, tile_out = refs
    del where_ref, marks_ref
    for a, ref in enumerate(blocks):
        tile_out[:, a * LANES : (a + 1) * LANES] = ref[0]
    row_count, _, g_rows, bands = both_ref.shape
    width = rotated_out.shape[1]
    pieces = tile_size // g_rows
    sums = jnp.zeros(rotated_out.shape, F32)
    for a in range(row_tiles):
        for r in range(0, row_count, 2):
            turn = jnp.concatenate(
                [
                    both_ref[q, 0, :, (a * pieces + s) * width : (a * pieces + s + 1) * width]
                    for q in (r, r + 1)
                    for s in range(pieces)
                ],
                axis=0,
            )
            at = (a * row_count + r) * tile_size
            sums = sums + over_k(psi_ref[:, at : at + 2 * tile_size], turn)
    rotated_out[...] = sums.astype(rotated_out.dtype)


def vmem():
    return pl.BlockSpec(memory_space=pltpu.VMEM)


def on_device(psi, hpsi, eigvec):
    g_rows, bands = psi.shape
    row_tiles, _, tile_size, col_tiles = eigvec.shape[:4]
    row_count = lax.axis_size("row")
    col_count = lax.axis_size("col")
    devices = row_count * col_count
    row_id = lax.axis_index("row")
    col_id = lax.axis_index("col")
    gvecs = g_rows * devices
    height = row_tiles * tile_size
    width = col_tiles * tile_size
    tiles = bands // tile_size
    where = jnp.stack([row_id, col_id]).astype(jnp.int32)

    lanes = bands // width
    folded = jnp.transpose(eigvec.reshape(lanes, g_rows, width), (1, 0, 2)).reshape(g_rows, bands)
    both = lax.all_gather(jnp.stack([psi, hpsi, folded]), "row")

    blocks_shape = jax.ShapeDtypeStruct((col_count, height, width), F32)
    strip_shape = jax.ShapeDtypeStruct((col_count, PB, width), F32)

    def products(body, source, kinds, with_head, made, name):
        def column_block(index, wide=tile_size):
            return pl.BlockSpec(
                (row_count, kinds, g_rows, wide), lambda c, where: (0, 0, 0, index(c, where))
            )

        in_specs = [
            column_block(lambda c, where, a=a: where[0] + a * row_count) for a in range(row_tiles)
        ]
        if with_head:
            in_specs.append(column_block(lambda c, where: 0))
            in_specs.append(column_block(lambda c, where: c, width))
        else:
            in_specs += [
                column_block(lambda c, where, a=a: c + a * col_count) for a in range(col_tiles)
            ]
        left = (height + PB * with_head, row_count * kinds * g_rows)
        return pl.pallas_call(
            body,
            out_shape=made,
            grid_spec=pltpu.PrefetchScalarGridSpec(
                num_scalar_prefetch=1,
                grid=(col_count,),
                in_specs=in_specs,
                out_specs=tuple(
                    pl.BlockSpec((1, *one.shape[1:]), lambda c, where: (c, 0, 0)) for one in made
                ),
                scratch_shapes=[pltpu.VMEM(left, psi.dtype)],
            ),
            compiler_params=pltpu.CompilerParams(vmem_limit_bytes=60 * MIB),
            name=name,
        )(where, *([source] * len(in_specs)))

    matrix, strip = products(
        functools.partial(matrix_body, row_tiles=row_tiles),
        both, 2, 1, (blocks_shape, strip_shape), "products",
    )

    summed = lax.psum(matrix, "col")
    strip = lax.all_to_all(strip, "col", 0, 0, tiled=True)
    strip = jnp.sum(strip, axis=0)
    strip = lax.all_to_all(
        jnp.broadcast_to(strip[None], strip_shape.shape), "col", 0, 0, tiled=True
    )
    (overlap,) = products(
        functools.partial(
            overlap_body, row_tiles=row_tiles, col_tiles=col_tiles, gvecs=gvecs
        ),
        both, 1, 0, (blocks_shape,), "overlaps",
    )
    panel = jnp.transpose(
        strip.reshape(row_tiles, col_count // row_tiles, PB, col_tiles, tile_size), (2, 1, 3, 0, 4)
    ).reshape(PB, tiles, tile_size)

    state = jax.ShapeDtypeStruct((PB, tiles, tile_size), F32)
    marks_shape = jax.ShapeDtypeStruct((8, tile_size), F32)

    def advance(peers, step, recv, vecs, images, marks, factor):
        return pl.pallas_call(
            functools.partial(step_body, row_count=row_count),
            out_shape=(
                state, state, marks_shape,
                jax.ShapeDtypeStruct((peers, row_tiles, tile_size), F32),
            ),
            in_specs=[pl.BlockSpec(memory_space=pltpu.SMEM)]
            + [vmem() for _ in range(6)],
            out_specs=tuple(vmem() for _ in range(4)),
            input_output_aliases={3: 0, 4: 1, 5: 2},
            compiler_params=pltpu.CompilerParams(vmem_limit_bytes=24 * MIB),
            name="reflect",
        )(jnp.reshape(step, (1,)).astype(jnp.int32), recv, panel, vecs, images, marks, factor)

    def wide(step, carry):
        vecs, images, marks, send = advance(devices, step, *carry, matrix)
        return lax.all_to_all(send, ("row", "col"), 0, 0, tiled=True), vecs, images, marks

    def narrow(step, carry):
        vecs, images, marks, send = advance(row_count, step, *carry, summed)
        return lax.all_to_all(send, "row", 0, 0, tiled=True), vecs, images, marks

    carry = (
        jnp.zeros((devices, row_tiles, tile_size), F32),
        jnp.zeros(state.shape, F32),
        jnp.zeros(state.shape, F32),
        jnp.zeros(marks_shape.shape, F32),
    )
    carry = lax.fori_loop(0, WIDE, wide, carry)
    psi, overlap, carry = lax.optimization_barrier((psi, overlap, carry))
    psi_rows = lax.all_gather(psi, "col", axis=0, tiled=True)
    correlation = lax.psum_scatter(overlap, "col", scatter_dimension=0, tiled=True)
    for step in range(WIDE, PB - 1):
        carry = narrow(jnp.int32(step), carry)
    def own_tile(a):
        def index(i, where):
            tile = where[1] + a * col_count
            return lax.div(tile, col_tiles), 0, lax.rem(tile, col_tiles)

        return pl.BlockSpec((1, height, tile_size), index)

    rotated, tile = pl.pallas_call(
        functools.partial(rotate_body, row_tiles=row_tiles, tile_size=tile_size),
        out_shape=(
            jax.ShapeDtypeStruct((g_rows * col_count, width), psi.dtype),
            jax.ShapeDtypeStruct((height, width), F32),
        ),
        grid_spec=pltpu.PrefetchScalarGridSpec(
            num_scalar_prefetch=1,
            grid=(1,),
            in_specs=[
                pl.BlockSpec((g_rows * col_count, bands), lambda i, where: (0, 0)),
                pl.BlockSpec((row_count, 1, g_rows, bands), lambda i, where: (0, 2, 0, 0)),
                pl.BlockSpec(marks_shape.shape, lambda i, where: (0, 0)),
            ]
            + [own_tile(a) for a in range(col_tiles)],
            out_specs=(
                pl.BlockSpec((g_rows * col_count, width), lambda i, where: (0, 0)),
                pl.BlockSpec((height, width), lambda i, where: (0, 0)),
            ),
        ),
        compiler_params=pltpu.CompilerParams(vmem_limit_bytes=60 * MIB),
        name="rotate",
    )(where, psi_rows, both, carry[3], *([summed] * col_tiles))
    recv, vecs, images, marks = narrow(jnp.int32(PB - 1), carry)

    updated = pl.pallas_call(
        functools.partial(last_body, row_count=row_count, col_count=col_count),
        out_shape=jax.ShapeDtypeStruct((height, width), F32),
        in_specs=[pl.BlockSpec(memory_space=pltpu.SMEM)] + [vmem() for _ in range(5)],
        out_specs=vmem(),
        scratch_shapes=[pltpu.VMEM(state.shape, F32), pltpu.VMEM(state.shape, F32)],
        compiler_params=pltpu.CompilerParams(vmem_limit_bytes=24 * MIB),
        name="update",
    )(where, recv, vecs, images, marks, tile)

    tile_shape = (row_tiles, 1, tile_size, col_tiles, 1, tile_size)
    return (
        correlation.reshape(tile_shape),
        updated.reshape(tile_shape),
        marks[0, :PB],
        marks[1, :PB],
        rotated.reshape(g_rows * col_count, col_tiles, 1, tile_size),
    )


def solution(mesh):
    return jax.shard_map(
        on_device,
        mesh=mesh,
        in_specs=(
            P(("row", "col"), None),
            P(("row", "col"), None),
            P(None, "row", None, None, "col", None),
        ),
        out_specs=(
            P(None, "row", None, None, "col", None),
            P(None, "row", None, None, "col", None),
            P(),
            P(),
            P("row", None, "col", None),
        ),
        check_vma=False,
    )
```

```python
import functools

import jax
import jax.numpy as jnp
from jax import lax
from jax.experimental import pallas as pl
from jax.experimental.pallas import tpu as pltpu
from jax.sharding import PartitionSpec as P

PB = 16
WIDE = 2
LANES = 128
F32 = jnp.float32
MIB = 1024 * 1024


def total(x):
    return jnp.sum(jnp.sum(x, axis=-2, keepdims=True), axis=-1, keepdims=True)


def over_k(left, right):
    return lax.dot_general(left, right, (((1,), (0,)), ((), ())), preferred_element_type=F32)


def matrix_body(where_ref, *refs, row_tiles, col_tiles):
    rows = refs[:row_tiles]
    head_ref = refs[row_tiles]
    cols = refs[row_tiles + 1 : row_tiles + 1 + col_tiles]
    matrix_out, strip_out, left_vmem = refs[row_tiles + 1 + col_tiles :]
    height = row_tiles * LANES

    def swapped(x):
        return jnp.concatenate([x[:, 1:2], x[:, 0:1]], axis=1).reshape(-1, LANES)

    @pl.when(pl.program_id(0) == 0)
    def _():
        for k, ref in enumerate(rows):
            left_vmem[pl.ds(k * LANES, LANES), :] = swapped(ref[...]).T
        left_vmem[height:, :] = swapped(head_ref[...]).T[:PB]

    both = jnp.concatenate([ref[...].reshape(-1, LANES) for ref in cols], axis=1)
    mixed = 0.5 * over_k(left_vmem[...], both)
    matrix_out[0] = mixed[:height]
    strip_out[0] = mixed[height:]


def overlap_body(where_ref, *refs, row_tiles, col_tiles, gvecs):
    rows = refs[:row_tiles]
    cols = refs[row_tiles : row_tiles + col_tiles]
    overlap_out, left_vmem = refs[row_tiles + col_tiles :]

    @pl.when(pl.program_id(0) == 0)
    def _():
        for k, ref in enumerate(rows):
            left_vmem[pl.ds(k * LANES, LANES), :] = ref[...].reshape(-1, LANES).T

    psi = jnp.concatenate([ref[...].reshape(-1, LANES) for ref in cols], axis=1)
    overlap_out[0] = over_k(left_vmem[...], psi) * (1.0 / gvecs)


def gathered(recv_ref, row_count):
    recv = recv_ref[...]
    count = recv.shape[0] // row_count
    if count > 1:
        recv = jnp.sum(recv.reshape(row_count, count, *recv.shape[1:]), axis=1)
    return recv.reshape(1, -1, LANES)


def finish_image(image, vecs, images, vector, tau):
    along_w = total(images * vector)
    along_v = total(vecs * vector)
    image = image - jnp.sum(vecs * along_w + images * along_v, axis=0, keepdims=True)
    image = tau * image
    return image - 0.5 * tau * total(image * vector) * vector


def place(into, what, slot):
    slots = lax.broadcasted_iota(jnp.int32, (PB, 1, 1), 0)
    return jnp.where(slots == slot, what, into)


def spot_of(tile, row_count, row_tiles):
    return (tile % row_count) * row_tiles + tile // row_count


def step_body(
    step_ref, recv_ref, panel_ref, vecs_ref, images_ref, marks_ref, matrix_ref,
    vecs_out, images_out, marks_out, send_out, *, row_count,
):
    step = step_ref[0]
    tiles = vecs_ref.shape[1]
    col_count, height, width = matrix_ref.shape
    row_tiles = height // LANES
    col_tiles = width // LANES
    lane = lax.broadcasted_iota(jnp.int32, (1, 1, LANES), 2)
    marks = marks_ref[...]
    vecs = vecs_ref[...]
    images = images_ref[...]
    before = jnp.maximum(step - 1, 0)
    vector = vecs_ref[pl.ds(before, 1)]
    tau = marks[2:3, 0:1].reshape(1, 1, 1)
    image = finish_image(gathered(recv_ref, row_count), vecs, images, vector, tau)
    images = place(images, image, step - 1)
    images_out[...] = images
    head_w = jnp.sum(jnp.where(lane == step, images[:, 0:1, :], 0.0), axis=-1, keepdims=True)
    head_v = jnp.sum(jnp.where(lane == step, vecs[:, 0:1, :], 0.0), axis=-1, keepdims=True)
    column = panel_ref[pl.ds(step, 1)] - jnp.sum(
        vecs * head_w + images * head_v, axis=0, keepdims=True
    )
    shape = (1, tiles, LANES)
    spot = lax.broadcasted_iota(jnp.int32, shape, 1)
    tile = lax.div(spot, row_tiles) + lax.rem(spot, row_tiles) * row_count
    positions = tile * LANES + lax.broadcasted_iota(jnp.int32, shape, 2)
    below = positions > step + 1
    pivot = total(jnp.where(positions == step + 1, column, 0.0))
    tail = total(jnp.where(below, column * column, 0.0))
    corner = total(jnp.where(positions == step, column, 0.0))
    length = jnp.sqrt(pivot * pivot + tail)
    beta = jnp.where(pivot >= 0.0, -length, length)
    tau = (beta - pivot) / beta
    vector = jnp.where(positions == step + 1, 1.0, jnp.where(below, column / (pivot - beta), 0.0))
    vecs_out[...] = place(vecs, vector, step)
    row = lax.broadcasted_iota(jnp.int32, marks.shape, 0)
    mark = lax.broadcasted_iota(jnp.int32, marks.shape, 1) == step
    flat = marks.shape
    marks = jnp.where((row == 0) & mark, jnp.broadcast_to(corner[0], flat), marks)
    marks = jnp.where((row == 1) & mark, jnp.broadcast_to(beta[0], flat), marks)
    marks_out[...] = jnp.where(row == 2, jnp.broadcast_to(tau[0], flat), marks)
    sums = jnp.zeros((height, LANES), F32)
    for c in range(col_count):
        for a in range(col_tiles):
            at = spot_of(a * col_count + c, row_count, row_tiles)
            sums = sums + matrix_ref[c, :, a * LANES : (a + 1) * LANES] * vector[0, at : at + 1, :]
    send = jnp.concatenate(
        [
            jnp.sum(sums[k * LANES : (k + 1) * LANES].T, axis=0, keepdims=True)
            for k in range(row_tiles)
        ],
        axis=0,
    )
    send_out[...] = jnp.broadcast_to(send[None], send_out.shape)


def last_body(
    where_ref, recv_ref, vecs_ref, images_ref, marks_ref, tile_ref,
    updated_out, vecs_vmem, images_vmem, *, row_count, col_count,
):
    row_id = where_ref[0]
    col_id = where_ref[1]
    height, width = updated_out.shape
    row_tiles = height // LANES
    col_tiles = width // LANES
    vecs = vecs_ref[...]
    vector = vecs_ref[PB - 1 : PB]
    tau = marks_ref[2:3, 0:1].reshape(1, 1, 1)
    image = finish_image(gathered(recv_ref, row_count), vecs, images_ref[...], vector, tau)
    images_vmem[...] = place(images_ref[...], image, PB - 1)
    vecs_vmem[...] = vecs

    def part(ref, tile):
        at = lax.rem(tile, row_count) * row_tiles + lax.div(tile, row_count)
        return ref[:, pl.ds(at, 1), :].reshape(PB, LANES)

    lefts = [
        jnp.concatenate([part(vecs_vmem, at), part(images_vmem, at)], axis=0)
        for at in (row_id + k * row_count for k in range(row_tiles))
    ]
    rights = [
        jnp.concatenate([part(images_vmem, at), part(vecs_vmem, at)], axis=0)
        for at in (col_id + k * col_count for k in range(col_tiles))
    ]
    left = jnp.concatenate(lefts, axis=1)
    right = jnp.concatenate(rights, axis=1)
    change = lax.dot_general(
        left, right, (((0,), (0,)), ((), ())),
        precision=lax.Precision.HIGHEST, preferred_element_type=F32,
    )
    updated_out[...] = tile_ref[...] - change


def rotate_body(
    where_ref, psi_ref, both_ref, marks_ref, block_ref, rotated_out, tile_out, *, row_tiles, tile_size
):
    del where_ref, marks_ref
    tile_out[...] = block_ref[0]
    row_count, _, g_rows, bands = both_ref.shape
    width = rotated_out.shape[1]
    pieces = tile_size // g_rows
    sums = jnp.zeros(rotated_out.shape, F32)
    for a in range(row_tiles):
        for r in range(0, row_count, 2):
            turn = jnp.concatenate(
                [
                    both_ref[q, 0, :, (a * pieces + s) * width : (a * pieces + s + 1) * width]
                    for q in (r, r + 1)
                    for s in range(pieces)
                ],
                axis=0,
            )
            at = (a * row_count + r) * tile_size
            sums = sums + over_k(psi_ref[:, at : at + 2 * tile_size], turn)
    rotated_out[...] = sums.astype(rotated_out.dtype)


def vmem():
    return pl.BlockSpec(memory_space=pltpu.VMEM)


def on_device(psi, hpsi, eigvec):
    g_rows, bands = psi.shape
    row_tiles, _, tile_size, col_tiles = eigvec.shape[:4]
    row_count = lax.axis_size("row")
    col_count = lax.axis_size("col")
    devices = row_count * col_count
    row_id = lax.axis_index("row")
    col_id = lax.axis_index("col")
    gvecs = g_rows * devices
    height = row_tiles * tile_size
    width = col_tiles * tile_size
    tiles = bands // tile_size
    where = jnp.stack([row_id, col_id]).astype(jnp.int32)

    lanes = bands // width
    folded = jnp.transpose(eigvec.reshape(lanes, g_rows, width), (1, 0, 2)).reshape(g_rows, bands)
    both = lax.all_gather(jnp.stack([psi, hpsi, folded]), "row")

    blocks_shape = jax.ShapeDtypeStruct((col_count, height, width), F32)
    strip_shape = jax.ShapeDtypeStruct((col_count, PB, width), F32)

    def products(body, source, kinds, with_head, made, name):
        def column_block(index):
            return pl.BlockSpec(
                (row_count, kinds, g_rows, tile_size), lambda c, where: (0, 0, 0, index(c, where))
            )

        in_specs = [
            column_block(lambda c, where, a=a: where[0] + a * row_count) for a in range(row_tiles)
        ]
        if with_head:
            in_specs.append(column_block(lambda c, where: 0))
        in_specs += [
            column_block(lambda c, where, a=a: c + a * col_count) for a in range(col_tiles)
        ]
        left = (height + PB * with_head, row_count * kinds * g_rows)
        return pl.pallas_call(
            body,
            out_shape=made,
            grid_spec=pltpu.PrefetchScalarGridSpec(
                num_scalar_prefetch=1,
                grid=(col_count,),
                in_specs=in_specs,
                out_specs=tuple(
                    pl.BlockSpec((1, *one.shape[1:]), lambda c, where: (c, 0, 0)) for one in made
                ),
                scratch_shapes=[pltpu.VMEM(left, psi.dtype)],
            ),
            compiler_params=pltpu.CompilerParams(vmem_limit_bytes=60 * MIB),
            name=name,
        )(where, *([source] * len(in_specs)))

    matrix, strip = products(
        functools.partial(matrix_body, row_tiles=row_tiles, col_tiles=col_tiles),
        both, 2, 1, (blocks_shape, strip_shape), "products",
    )

    summed = lax.psum(matrix, "col")
    strip = lax.all_to_all(strip, "col", 0, 0, tiled=True)
    strip = jnp.sum(strip, axis=0)
    strip = lax.all_to_all(
        jnp.broadcast_to(strip[None], strip_shape.shape), "col", 0, 0, tiled=True
    )
    (overlap,) = products(
        functools.partial(
            overlap_body, row_tiles=row_tiles, col_tiles=col_tiles, gvecs=gvecs
        ),
        both, 1, 0, (blocks_shape,), "overlaps",
    )
    panel = jnp.transpose(
        strip.reshape(col_count, PB, row_tiles, col_tiles // row_tiles, tile_size), (1, 3, 0, 2, 4)
    ).reshape(PB, tiles, tile_size)

    state = jax.ShapeDtypeStruct((PB, tiles, tile_size), F32)
    marks_shape = jax.ShapeDtypeStruct((8, tile_size), F32)

    def advance(peers, step, recv, vecs, images, marks, factor):
        return pl.pallas_call(
            functools.partial(step_body, row_count=row_count),
            out_shape=(
                state, state, marks_shape,
                jax.ShapeDtypeStruct((peers, row_tiles, tile_size), F32),
            ),
            in_specs=[pl.BlockSpec(memory_space=pltpu.SMEM)]
            + [vmem() for _ in range(6)],
            out_specs=tuple(vmem() for _ in range(4)),
            input_output_aliases={3: 0, 4: 1, 5: 2},
            compiler_params=pltpu.CompilerParams(vmem_limit_bytes=24 * MIB),
            name="reflect",
        )(jnp.reshape(step, (1,)).astype(jnp.int32), recv, panel, vecs, images, marks, factor)

    def wide(step, carry):
        vecs, images, marks, send = advance(devices, step, *carry, matrix)
        return lax.all_to_all(send, ("row", "col"), 0, 0, tiled=True), vecs, images, marks

    def narrow(step, carry):
        vecs, images, marks, send = advance(row_count, step, *carry, summed)
        return lax.all_to_all(send, "row", 0, 0, tiled=True), vecs, images, marks

    carry = (
        jnp.zeros((devices, row_tiles, tile_size), F32),
        jnp.zeros(state.shape, F32),
        jnp.zeros(state.shape, F32),
        jnp.zeros(marks_shape.shape, F32),
    )
    carry = lax.fori_loop(0, WIDE, wide, carry)
    psi, overlap, carry = lax.optimization_barrier((psi, overlap, carry))
    psi_rows = lax.all_gather(psi, "col", axis=0, tiled=True)
    correlation = lax.psum_scatter(overlap, "col", scatter_dimension=0, tiled=True)
    for step in range(WIDE, PB - 1):
        carry = narrow(jnp.int32(step), carry)
    rotated, tile = pl.pallas_call(
        functools.partial(rotate_body, row_tiles=row_tiles, tile_size=tile_size),
        out_shape=(
            jax.ShapeDtypeStruct((g_rows * col_count, width), psi.dtype),
            jax.ShapeDtypeStruct((height, width), F32),
        ),
        grid_spec=pltpu.PrefetchScalarGridSpec(
            num_scalar_prefetch=1,
            grid=(1,),
            in_specs=[
                pl.BlockSpec((g_rows * col_count, bands), lambda i, where: (0, 0)),
                pl.BlockSpec((row_count, 1, g_rows, bands), lambda i, where: (0, 2, 0, 0)),
                pl.BlockSpec(marks_shape.shape, lambda i, where: (0, 0)),
                pl.BlockSpec((1, height, width), lambda i, where: (where[1], 0, 0)),
            ],
            out_specs=(
                pl.BlockSpec((g_rows * col_count, width), lambda i, where: (0, 0)),
                pl.BlockSpec((height, width), lambda i, where: (0, 0)),
            ),
        ),
        compiler_params=pltpu.CompilerParams(vmem_limit_bytes=48 * MIB),
        name="rotate",
    )(where, psi_rows, both, carry[3], summed)
    recv, vecs, images, marks = narrow(jnp.int32(PB - 1), carry)

    updated = pl.pallas_call(
        functools.partial(last_body, row_count=row_count, col_count=col_count),
        out_shape=jax.ShapeDtypeStruct((height, width), F32),
        in_specs=[pl.BlockSpec(memory_space=pltpu.SMEM)] + [vmem() for _ in range(5)],
        out_specs=vmem(),
        scratch_shapes=[pltpu.VMEM(state.shape, F32), pltpu.VMEM(state.shape, F32)],
        compiler_params=pltpu.CompilerParams(vmem_limit_bytes=24 * MIB),
        name="update",
    )(where, recv, vecs, images, marks, tile)

    tile_shape = (row_tiles, 1, tile_size, col_tiles, 1, tile_size)
    return (
        correlation.reshape(tile_shape),
        updated.reshape(tile_shape),
        marks[0, :PB],
        marks[1, :PB],
        rotated.reshape(g_rows * col_count, col_tiles, 1, tile_size),
    )


def solution(mesh):
    return jax.shard_map(
        on_device,
        mesh=mesh,
        in_specs=(
            P(("row", "col"), None),
            P(("row", "col"), None),
            P(None, "row", None, None, "col", None),
        ),
        out_specs=(
            P(None, "row", None, None, "col", None),
            P(None, "row", None, None, "col", None),
            P(),
            P(),
            P("row", None, "col", None),
        ),
        check_vma=False,
    )
```

```python
import functools

import jax
import jax.numpy as jnp
from jax import lax
from jax.experimental import pallas as pl
from jax.experimental.pallas import tpu as pltpu
from jax.sharding import PartitionSpec as P

PB = 16
WIDE = 2
LANES = 128
F32 = jnp.float32
MIB = 1024 * 1024


def total(x):
    return jnp.sum(jnp.sum(x, axis=-2, keepdims=True), axis=-1, keepdims=True)


def over_k(left, right):
    return lax.dot_general(left, right, (((1,), (0,)), ((), ())), preferred_element_type=F32)


def matrix_body(where_ref, *refs, row_tiles, col_tiles):
    rows = refs[:row_tiles]
    head_ref = refs[row_tiles]
    cols = refs[row_tiles + 1 : row_tiles + 1 + col_tiles]
    matrix_out, strip_out, left_vmem = refs[row_tiles + 1 + col_tiles :]
    height = row_tiles * LANES

    def swapped(x):
        return jnp.concatenate([x[:, 1:2], x[:, 0:1]], axis=1).reshape(-1, LANES)

    @pl.when(pl.program_id(0) == 0)
    def _():
        for k, ref in enumerate(rows):
            left_vmem[pl.ds(k * LANES, LANES), :] = swapped(ref[...]).T
        left_vmem[height:, :] = swapped(head_ref[...]).T[:PB]

    both = jnp.concatenate([ref[...].reshape(-1, LANES) for ref in cols], axis=1)
    mixed = 0.5 * over_k(left_vmem[...], both)
    matrix_out[0] = mixed[:height]
    strip_out[0] = mixed[height:]


def overlap_body(where_ref, *refs, row_tiles, col_tiles, gvecs):
    rows = refs[:row_tiles]
    cols = refs[row_tiles : row_tiles + col_tiles]
    overlap_out, left_vmem = refs[row_tiles + col_tiles :]

    @pl.when(pl.program_id(0) == 0)
    def _():
        for k, ref in enumerate(rows):
            left_vmem[pl.ds(k * LANES, LANES), :] = ref[...].reshape(-1, LANES).T

    psi = jnp.concatenate([ref[...].reshape(-1, LANES) for ref in cols], axis=1)
    overlap_out[0] = over_k(left_vmem[...], psi) * (1.0 / gvecs)


def gathered(recv_ref, row_count):
    recv = recv_ref[...]
    count = recv.shape[0] // row_count
    if count > 1:
        recv = jnp.sum(recv.reshape(row_count, count, *recv.shape[1:]), axis=1)
    return recv.reshape(1, -1, LANES)


def finish_image(image, vecs, images, vector, tau):
    along_w = total(images * vector)
    along_v = total(vecs * vector)
    image = image - jnp.sum(vecs * along_w + images * along_v, axis=0, keepdims=True)
    image = tau * image
    return image - 0.5 * tau * total(image * vector) * vector


def place(into, what, slot):
    slots = lax.broadcasted_iota(jnp.int32, (PB, 1, 1), 0)
    return jnp.where(slots == slot, what, into)


def spot_of(tile, row_count, row_tiles):
    return (tile % row_count) * row_tiles + tile // row_count


def step_body(
    step_ref, recv_ref, panel_ref, vecs_ref, images_ref, marks_ref, matrix_ref,
    vecs_out, images_out, marks_out, send_out, *, row_count,
):
    step = step_ref[0]
    tiles = vecs_ref.shape[1]
    col_count, height, width = matrix_ref.shape
    row_tiles = height // LANES
    col_tiles = width // LANES
    lane = lax.broadcasted_iota(jnp.int32, (1, 1, LANES), 2)
    marks = marks_ref[...]
    vecs = vecs_ref[...]
    images = images_ref[...]
    before = jnp.maximum(step - 1, 0)
    vector = vecs_ref[pl.ds(before, 1)]
    tau = marks[2:3, 0:1].reshape(1, 1, 1)
    image = finish_image(gathered(recv_ref, row_count), vecs, images, vector, tau)
    images = place(images, image, step - 1)
    images_out[...] = images
    head_w = jnp.sum(jnp.where(lane == step, images[:, 0:1, :], 0.0), axis=-1, keepdims=True)
    head_v = jnp.sum(jnp.where(lane == step, vecs[:, 0:1, :], 0.0), axis=-1, keepdims=True)
    column = panel_ref[pl.ds(step, 1)] - jnp.sum(
        vecs * head_w + images * head_v, axis=0, keepdims=True
    )
    shape = (1, tiles, LANES)
    spot = lax.broadcasted_iota(jnp.int32, shape, 1)
    tile = lax.div(spot, row_tiles) + lax.rem(spot, row_tiles) * row_count
    positions = tile * LANES + lax.broadcasted_iota(jnp.int32, shape, 2)
    below = positions > step + 1
    pivot = total(jnp.where(positions == step + 1, column, 0.0))
    tail = total(jnp.where(below, column * column, 0.0))
    corner = total(jnp.where(positions == step, column, 0.0))
    length = jnp.sqrt(pivot * pivot + tail)
    beta = jnp.where(pivot >= 0.0, -length, length)
    tau = (beta - pivot) / beta
    vector = jnp.where(positions == step + 1, 1.0, jnp.where(below, column / (pivot - beta), 0.0))
    vecs_out[...] = place(vecs, vector, step)
    row = lax.broadcasted_iota(jnp.int32, marks.shape, 0)
    mark = lax.broadcasted_iota(jnp.int32, marks.shape, 1) == step
    flat = marks.shape
    marks = jnp.where((row == 0) & mark, jnp.broadcast_to(corner[0], flat), marks)
    marks = jnp.where((row == 1) & mark, jnp.broadcast_to(beta[0], flat), marks)
    marks_out[...] = jnp.where(row == 2, jnp.broadcast_to(tau[0], flat), marks)
    sums = jnp.zeros((height, LANES), F32)
    for c in range(col_count):
        for a in range(col_tiles):
            at = spot_of(a * col_count + c, row_count, row_tiles)
            sums = sums + matrix_ref[c, :, a * LANES : (a + 1) * LANES] * vector[0, at : at + 1, :]
    send = jnp.concatenate(
        [
            jnp.sum(sums[k * LANES : (k + 1) * LANES].T, axis=0, keepdims=True)
            for k in range(row_tiles)
        ],
        axis=0,
    )
    send_out[...] = jnp.broadcast_to(send[None], send_out.shape)


def last_body(
    where_ref, recv_ref, vecs_ref, images_ref, marks_ref, tile_ref,
    updated_out, vecs_vmem, images_vmem, *, row_count, col_count,
):
    row_id = where_ref[0]
    col_id = where_ref[1]
    height, width = updated_out.shape
    row_tiles = height // LANES
    col_tiles = width // LANES
    vecs = vecs_ref[...]
    vector = vecs_ref[PB - 1 : PB]
    tau = marks_ref[2:3, 0:1].reshape(1, 1, 1)
    image = finish_image(gathered(recv_ref, row_count), vecs, images_ref[...], vector, tau)
    images_vmem[...] = place(images_ref[...], image, PB - 1)
    vecs_vmem[...] = vecs

    def part(ref, tile):
        at = lax.rem(tile, row_count) * row_tiles + lax.div(tile, row_count)
        return ref[:, pl.ds(at, 1), :].reshape(PB, LANES)

    lefts = [
        jnp.concatenate([part(vecs_vmem, at), part(images_vmem, at)], axis=0)
        for at in (row_id + k * row_count for k in range(row_tiles))
    ]
    rights = [
        jnp.concatenate([part(images_vmem, at), part(vecs_vmem, at)], axis=0)
        for at in (col_id + k * col_count for k in range(col_tiles))
    ]
    left = jnp.concatenate(lefts, axis=1)
    right = jnp.concatenate(rights, axis=1)
    change = lax.dot_general(
        left, right, (((0,), (0,)), ((), ())),
        precision=lax.Precision.HIGHEST, preferred_element_type=F32,
    )
    updated_out[...] = tile_ref[...] - change


def rotate_body(
    where_ref, psi_ref, both_ref, marks_ref, block_ref, rotated_out, tile_out, *, row_tiles, tile_size
):
    del where_ref, marks_ref
    tile_out[...] = block_ref[0]
    row_count, _, g_rows, bands = both_ref.shape
    width = rotated_out.shape[1]
    pieces = tile_size // g_rows
    sums = jnp.zeros(rotated_out.shape, F32)
    for a in range(row_tiles):
        for r in range(0, row_count, 2):
            turn = jnp.concatenate(
                [
                    both_ref[q, 0, :, (a * pieces + s) * width : (a * pieces + s + 1) * width]
                    for q in (r, r + 1)
                    for s in range(pieces)
                ],
                axis=0,
            )
            at = (a * row_count + r) * tile_size
            sums = sums + over_k(psi_ref[:, at : at + 2 * tile_size], turn)
    rotated_out[...] = sums.astype(rotated_out.dtype)


def vmem():
    return pl.BlockSpec(memory_space=pltpu.VMEM)


def on_device(psi, hpsi, eigvec):
    g_rows, bands = psi.shape
    row_tiles, _, tile_size, col_tiles = eigvec.shape[:4]
    row_count = lax.axis_size("row")
    col_count = lax.axis_size("col")
    devices = row_count * col_count
    row_id = lax.axis_index("row")
    col_id = lax.axis_index("col")
    gvecs = g_rows * devices
    height = row_tiles * tile_size
    width = col_tiles * tile_size
    tiles = bands // tile_size
    where = jnp.stack([row_id, col_id]).astype(jnp.int32)

    lanes = bands // width
    folded = jnp.transpose(eigvec.reshape(lanes, g_rows, width), (1, 0, 2)).reshape(g_rows, bands)
    both = lax.all_gather(jnp.stack([psi, hpsi, folded]), "row")

    blocks_shape = jax.ShapeDtypeStruct((col_count, height, width), F32)
    strip_shape = jax.ShapeDtypeStruct((col_count, PB, width), F32)

    def products(body, source, kinds, with_head, made, name):
        def column_block(index):
            return pl.BlockSpec(
                (row_count, kinds, g_rows, tile_size), lambda c, where: (0, 0, 0, index(c, where))
            )

        in_specs = [
            column_block(lambda c, where, a=a: where[0] + a * row_count) for a in range(row_tiles)
        ]
        if with_head:
            in_specs.append(column_block(lambda c, where: 0))
        in_specs += [
            column_block(lambda c, where, a=a: c + a * col_count) for a in range(col_tiles)
        ]
        left = (height + PB * with_head, row_count * kinds * g_rows)
        return pl.pallas_call(
            body,
            out_shape=made,
            grid_spec=pltpu.PrefetchScalarGridSpec(
                num_scalar_prefetch=1,
                grid=(col_count,),
                in_specs=in_specs,
                out_specs=tuple(
                    pl.BlockSpec((1, *one.shape[1:]), lambda c, where: (c, 0, 0)) for one in made
                ),
                scratch_shapes=[pltpu.VMEM(left, psi.dtype)],
            ),
            compiler_params=pltpu.CompilerParams(vmem_limit_bytes=60 * MIB),
            name=name,
        )(where, *([source] * len(in_specs)))

    matrix, strip = products(
        functools.partial(matrix_body, row_tiles=row_tiles, col_tiles=col_tiles),
        both, 2, 1, (blocks_shape, strip_shape), "products",
    )

    summed = lax.psum(matrix, "col")
    strip = lax.all_to_all(strip, "col", 0, 0, tiled=True)
    strip = jnp.sum(strip, axis=0)
    strip = lax.all_to_all(
        jnp.broadcast_to(strip[None], strip_shape.shape), "col", 0, 0, tiled=True
    )
    (overlap,) = products(
        functools.partial(
            overlap_body, row_tiles=row_tiles, col_tiles=col_tiles, gvecs=gvecs
        ),
        both, 1, 0, (blocks_shape,), "overlaps",
    )
    panel = jnp.transpose(
        strip.reshape(col_count, PB, row_tiles, col_tiles // row_tiles, tile_size), (1, 3, 0, 2, 4)
    ).reshape(PB, tiles, tile_size)

    state = jax.ShapeDtypeStruct((PB, tiles, tile_size), F32)
    marks_shape = jax.ShapeDtypeStruct((8, tile_size), F32)

    def advance(peers, step, recv, vecs, images, marks, factor):
        return pl.pallas_call(
            functools.partial(step_body, row_count=row_count),
            out_shape=(
                state, state, marks_shape,
                jax.ShapeDtypeStruct((peers, row_tiles, tile_size), F32),
            ),
            in_specs=[pl.BlockSpec(memory_space=pltpu.SMEM)]
            + [vmem() for _ in range(6)],
            out_specs=tuple(vmem() for _ in range(4)),
            input_output_aliases={3: 0, 4: 1, 5: 2},
            compiler_params=pltpu.CompilerParams(vmem_limit_bytes=24 * MIB),
            name="reflect",
        )(jnp.reshape(step, (1,)).astype(jnp.int32), recv, panel, vecs, images, marks, factor)

    def wide(step, carry):
        vecs, images, marks, send = advance(devices, step, *carry, matrix)
        return lax.all_to_all(send, ("row", "col"), 0, 0, tiled=True), vecs, images, marks

    def narrow(step, carry):
        vecs, images, marks, send = advance(row_count, step, *carry, summed)
        return lax.all_to_all(send, "row", 0, 0, tiled=True), vecs, images, marks

    carry = (
        jnp.zeros((devices, row_tiles, tile_size), F32),
        jnp.zeros(state.shape, F32),
        jnp.zeros(state.shape, F32),
        jnp.zeros(marks_shape.shape, F32),
    )
    carry = lax.fori_loop(0, WIDE, wide, carry)
    psi, overlap, carry = lax.optimization_barrier((psi, overlap, carry))
    psi_rows = lax.all_gather(psi, "col", axis=0, tiled=True)
    correlation = lax.psum_scatter(overlap, "col", scatter_dimension=0, tiled=True)
    for step in range(WIDE, PB - 1):
        carry = narrow(jnp.int32(step), carry)
    rotated, tile = pl.pallas_call(
        functools.partial(rotate_body, row_tiles=row_tiles, tile_size=tile_size),
        out_shape=(
            jax.ShapeDtypeStruct((g_rows * col_count, width), psi.dtype),
            jax.ShapeDtypeStruct((height, width), F32),
        ),
        grid_spec=pltpu.PrefetchScalarGridSpec(
            num_scalar_prefetch=1,
            grid=(1,),
            in_specs=[
                pl.BlockSpec((g_rows * col_count, bands), lambda i, where: (0, 0)),
                pl.BlockSpec((row_count, 1, g_rows, bands), lambda i, where: (0, 2, 0, 0)),
                pl.BlockSpec(marks_shape.shape, lambda i, where: (0, 0)),
                pl.BlockSpec((1, height, width), lambda i, where: (where[1], 0, 0)),
            ],
            out_specs=(
                pl.BlockSpec((g_rows * col_count, width), lambda i, where: (0, 0)),
                pl.BlockSpec((height, width), lambda i, where: (0, 0)),
            ),
        ),
        compiler_params=pltpu.CompilerParams(vmem_limit_bytes=48 * MIB),
        name="rotate",
    )(where, psi_rows, both, carry[3], summed)
    recv, vecs, images, marks = narrow(jnp.int32(PB - 1), carry)

    tile_shape = (row_tiles, 1, tile_size, col_tiles, 1, tile_size)
    tile, correlation = lax.optimization_barrier((tile, correlation.reshape(tile_shape)))
    updated = pl.pallas_call(
        functools.partial(last_body, row_count=row_count, col_count=col_count),
        out_shape=jax.ShapeDtypeStruct((height, width), F32),
        in_specs=[pl.BlockSpec(memory_space=pltpu.SMEM)] + [vmem() for _ in range(5)],
        out_specs=vmem(),
        scratch_shapes=[pltpu.VMEM(state.shape, F32), pltpu.VMEM(state.shape, F32)],
        compiler_params=pltpu.CompilerParams(vmem_limit_bytes=24 * MIB),
        name="update",
    )(where, recv, vecs, images, marks, tile)

    tile_shape = (row_tiles, 1, tile_size, col_tiles, 1, tile_size)
    return (
        correlation,
        updated.reshape(tile_shape),
        marks[0, :PB],
        marks[1, :PB],
        rotated.reshape(g_rows * col_count, col_tiles, 1, tile_size),
    )


def solution(mesh):
    return jax.shard_map(
        on_device,
        mesh=mesh,
        in_specs=(
            P(("row", "col"), None),
            P(("row", "col"), None),
            P(None, "row", None, None, "col", None),
        ),
        out_specs=(
            P(None, "row", None, None, "col", None),
            P(None, "row", None, None, "col", None),
            P(),
            P(),
            P("row", None, "col", None),
        ),
        check_vma=False,
    )
```
